256 devices in a mesh: batch: 8 (over z), mp: 32 (over x, y, core).
Axes of the slice: x: 4, y: 4, z: 8, core: 2. Of those that a mesh axis runs over, the one named last changes fastest.
Arguments:
- stream: bfloat16 [256, 8192], P(None, 'mp'), may hold values from -6 to 6
- input_gain: float32 [8192], P('mp'), may hold values from 0.5 to 1.5
- query_bias: float32 [8192], P('batch'), may hold values from -3 to 3
- query_weight: bfloat16 [8192, 8192], P('mp', 'batch'), may hold values from -0.0625 to 0.0625
- out_weight: bfloat16 [8192, 8192], P('batch', 'mp'), may hold values from -6 to 6
- page_cache: bfloat16 [2, 8, 2048, 128, 128], P(None, 'batch', 'mp'), may hold values from -43 to 43
- page_table: int32 [256, 24], P('mp'), may hold values from 0 to 63, as said below
- lengths: int32 [256], P('mp'), may hold values from 1 to 3072, as said below
- final_gain: float32 [8192], P('mp'), may hold values from 0.5 to 1.5
- head_weight: bfloat16 [8192, 98304], P('mp', 'batch'), may hold values from -11 to 11
Outputs:
- logits: float32 [256, 98304], P(None, ('batch', 'mp'))
- log_norm: float32 [256], replicated
The draws below stay inside these ranges and needn't reach their ends.
Inputs may be any that keep to these rules, and one draw needn't show every extreme that they name: Each sequence's pages are the first ceil(lengths / 128) entries of its row of page_table; together the sequences of one index of mp use at most 64 pages; some sequence holds exactly 3072 tokens. `page_table`: entries are slots of the pool of the index of mp that holds the sequence; the live entries (the first ceil(lengths / 128) of each row) of all rows of one index of mp are distinct; later entries are arbitrary slots.
All inputs are finite; a program needn't handle non-finite values.
Results may differ from the reference program's by a relative error of at most 0.0099.
Values may be sent and summed in bfloat16 or wider, within the bound.
No kernel may reach another device: no remote copies, remote signals or barrier semaphores. Data moves between devices by JAX's collectives and lax.ppermute only.
A program may use at most 128 MiB of HBM per device.

```python
import math
from functools import partial
import jax
import jax.numpy as jnp
from jax import lax

D = 8192
HEADS = 64
KV_HEADS = 8
HEAD_DIM = 128
VOCAB = 98304
PAGE = 128
MAX_PAGES = 24
SEQ_DEV = 8
SEQS = 256
POOL = 64


def rising(count, factor):
    steps = jnp.arange(count, dtype=jnp.float32) / max(count - 1, 1)
    return factor ** (0.5 * steps)


def draw_stream(key, part):
    column_scale = 0.5 * rising(D, 3.0)
    samples = jnp.clip(jax.random.normal(key, (SEQS, D), jnp.float32), -6.0, 6.0)
    return (samples * column_scale[None, :]).astype(jnp.bfloat16)


def draw_out_weight(key, part):
    column_scale = 8.0 / math.sqrt(HEADS * HEAD_DIM) * rising(D, 3.0)
    samples = jnp.clip(jax.random.normal(key, (HEADS * HEAD_DIM, D), jnp.float32), -6.0, 6.0)
    return (samples * column_scale[None, :]).astype(jnp.bfloat16)


def draw_page_cache(key, part):
    extent = (2, KV_HEADS, SEQS // SEQ_DEV * POOL, PAGE, HEAD_DIM)
    sample_key = jax.random.fold_in(key, 0)
    samples = jnp.clip(jax.random.normal(sample_key, extent, jnp.float32), -6.0, 6.0)
    return samples.astype(jnp.bfloat16)


def draw_head_weight(key, part):
    sample_key = jax.random.fold_in(key, 0)
    column_scale = 4.0 / math.sqrt(D) * (0.8 + 0.4 * jnp.arange(VOCAB, dtype=jnp.float32) / VOCAB)
    samples = jnp.clip(jax.random.normal(sample_key, (D, VOCAB), jnp.float32), -6.0, 6.0)
    return (samples * column_scale[None, :]).astype(jnp.bfloat16)


def page_plan(key):
    blocks = SEQS // SEQ_DEV
    base_key = jax.random.fold_in(key, 7)
    weight_key, long_key, fill_key, shuffle_key, spare_key = jax.random.split(base_key, 5)
    weights = jax.random.randint(weight_key, (blocks, SEQ_DEV), 1, 33) ** 2
    spare_pages = POOL - MAX_PAGES - SEQ_DEV + 1
    counts = jnp.minimum(1 + weights * spare_pages // jnp.sum(weights, axis=1, keepdims=True), MAX_PAGES)
    sequence_ids = jnp.arange(SEQS, dtype=jnp.int32)
    longest = jax.random.randint(long_key, (), 0, SEQS)
    counts = jnp.where(sequence_ids == longest, MAX_PAGES, counts.reshape(SEQS)).astype(jnp.int32)
    last_fill = jax.random.randint(fill_key, (SEQS,), 1, PAGE + 1)
    last_fill = jnp.where(sequence_ids == longest, PAGE, last_fill)
    lengths = ((counts - 1) * PAGE + last_fill).astype(jnp.int32)
    grouped = counts.reshape(blocks, SEQ_DEV)
    starts = jnp.cumsum(grouped, axis=1) - grouped
    shuffles = jax.vmap(partial(jax.random.permutation, x=POOL))(jax.random.split(shuffle_key, blocks))
    page_order = jnp.arange(MAX_PAGES, dtype=jnp.int32)
    position = jnp.minimum(starts[:, :, None] + page_order[None, None, :], POOL - 1)
    spread = jnp.broadcast_to(shuffles[:, None, :], (blocks, SEQ_DEV, POOL))
    chosen = jnp.take_along_axis(spread, position, axis=2)
    filler = jax.random.randint(spare_key, (blocks, SEQ_DEV, MAX_PAGES), 0, POOL)
    slot_table = jnp.where(page_order[None, None, :] < grouped[:, :, None], chosen, filler)
    return (lengths, slot_table.reshape(SEQS, MAX_PAGES).astype(jnp.int32))


def draw_lengths(key, part):
    return page_plan(key)[0]


def draw_page_table(key, part):
    return page_plan(key)[1]


def block_levels(rng, shape, cuts, low, top_value):
    loudness = 1.0
    for axis_at, shards_of in cuts:
        draws = jax.random.uniform(jax.random.fold_in(jax.random.fold_in(rng, 6), axis_at), (shards_of,), jnp.float32, low / len(cuts), top_value / len(cuts))
        loudness = loudness * jnp.repeat(jnp.exp(draws), shape[axis_at] // shards_of).reshape((-1,) + (1,) * (len(shape) - 1 - axis_at))
    return loudness


def normal_values(stream_key, dims, scale, limit, shards=(), kind=jnp.bfloat16):
    values = scale * jax.random.normal(stream_key, dims, jnp.float32)
    if shards:
        values = values * block_levels(stream_key, dims, shards, -0.22, 0.18)
    return jnp.clip(values, -limit, limit).astype(kind)


def setup_inputs(seed: int = 0) -> dict:
    keys = jax.random.split(jax.random.key(seed), 11)
    stream = draw_stream(jax.random.fold_in(keys[10], 71), 0)
    input_gain = jnp.clip(1.0 + 0.1 * jax.random.normal(keys[1], (D,), jnp.float32), 0.5, 1.5)
    query_bias = normal_values(keys[2], (HEADS * HEAD_DIM,), 0.5, 3.0, ((0, 8),), jnp.float32)
    query_weight = normal_values(keys[3], (D, HEADS * HEAD_DIM), D ** -0.5, 0.0625, ((0, 32), (1, 8)))
    out_weight = draw_out_weight(jax.random.fold_in(keys[10], 71), 0)
    page_cache = draw_page_cache(jax.random.fold_in(keys[10], 71), 0)
    page_table = draw_page_table(jax.random.fold_in(keys[10], 71), 0)
    lengths = draw_lengths(jax.random.fold_in(keys[10], 71), 0)
    final_gain = jnp.clip(1.0 + 0.1 * jax.random.normal(keys[8], (D,), jnp.float32), 0.5, 1.5)
    head_weight = draw_head_weight(jax.random.fold_in(keys[10], 71), 0)
    return dict(stream=stream, input_gain=input_gain, query_bias=query_bias, query_weight=query_weight, out_weight=out_weight, page_cache=page_cache, page_table=page_table, lengths=lengths, final_gain=final_gain, head_weight=head_weight)


EPS = 1e-06
ROPE_BASE = 1000000.0

def normalize(features, gain, squares, full_width):
    return features * lax.rsqrt(squares[:, None] / full_width + EPS) * gain

def rotate(queries, position):
    head_size = queries.shape[-1]
    half_dim = head_size // 2
    exponent = jnp.arange(half_dim, dtype=jnp.float32) * (-2.0 / head_size)
    frequency = ROPE_BASE ** exponent
    angles = position.astype(jnp.float32)[:, None] * frequency[None, :]
    cosines = jnp.cos(angles)[:, None, :]
    sines = jnp.sin(angles)[:, None, :]
    leading = queries[..., :half_dim]
    trailing = queries[..., half_dim:]
    return jnp.concatenate([leading * cosines - trailing * sines, trailing * cosines + leading * sines], axis=-1)

def reference(stream, input_gain, query_bias, query_weight, out_weight, page_cache, page_table, lengths, final_gain, head_weight):
    features = stream.astype(jnp.float32)
    normed = normalize(features, input_gain, lax.optimization_barrier(jnp.sum(features * features, axis=1)), D).astype(jnp.bfloat16)
    queries = jnp.dot(normed, query_weight, preferred_element_type=jnp.float32) + query_bias
    queries = rotate(queries.reshape(SEQS, HEADS, HEAD_DIM), lengths - 1).astype(jnp.bfloat16)
    per_group = HEADS // KV_HEADS
    span = MAX_PAGES * PAGE
    blocks = (jnp.arange(SEQS, dtype=jnp.int32) // SEQ_DEV).astype(jnp.int32)

    def one_sequence(item):
        query_row, table_row, length, block = item
        slots = (block * POOL + table_row).astype(jnp.int32)
        gathered = jnp.take(page_cache, slots, axis=2).astype(jnp.float32)
        gathered = gathered.reshape(2, KV_HEADS, span, HEAD_DIM)
        grouped = query_row.astype(jnp.float32).reshape(KV_HEADS, per_group, HEAD_DIM)
        scores = jnp.einsum('hgd,htd->hgt', grouped, gathered[0]) / math.sqrt(HEAD_DIM)
        visible = jnp.arange(span, dtype=jnp.int32) < length
        scores = jnp.where(visible, scores, -1e+30)
        highest = lax.optimization_barrier(jnp.max(scores, axis=2, keepdims=True))
        powers = jnp.where(visible, jnp.exp(scores - highest), 0.0)
        weights = (powers / lax.optimization_barrier(jnp.sum(powers, axis=2, keepdims=True))).astype(jnp.bfloat16)
        result = jnp.einsum('hgt,htd->hgd', weights.astype(jnp.float32), gathered[1])
        return result.reshape(HEADS * HEAD_DIM).astype(jnp.bfloat16)
    attended = lax.map(one_sequence, (queries, page_table, lengths, blocks))
    residual = features + jnp.dot(attended, out_weight, preferred_element_type=jnp.float32)
    normed_out = normalize(residual, final_gain, lax.optimization_barrier(jnp.sum(residual * residual, axis=1)), D).astype(jnp.bfloat16)
    logits = jnp.dot(normed_out, head_weight, preferred_element_type=jnp.float32)
    highest = lax.optimization_barrier(jnp.max(logits, axis=1))
    log_norm = jnp.log(lax.optimization_barrier(jnp.sum(jnp.exp(logits - highest[:, None]), axis=1))) + highest
    return (logits, log_norm)
```

```python
import math

import jax
import jax.numpy as jnp
from jax import lax
from jax.experimental import pallas as pl
from jax.experimental.pallas import tpu as pltpu
from jax.sharding import Mesh
from jax.sharding import PartitionSpec as P

MP = ("mp_0", "mp_1", "mp_2")
BATCH_MP = ("batch", "mp_0", "mp_1", "mp_2")
XY = ("mp_0", "mp_1")
BATCH_CORE = ("batch", "mp_2")


EPS = 1e-06
ROPE_BASE = 1000000.0
INTERPRET = False

LANES = 128


def sent_to_all(x, axis):
    length = lax.axis_size(axis)
    return lax.all_to_all(jnp.broadcast_to(x[None], (length, *x.shape)), axis, 0, 0, tiled=True)


def shifted(x, axis, by):
    length = lax.axis_size(axis)
    return lax.ppermute(x, axis, [(k, (k + by) % length) for k in range(length)])


def halves(x):
    coarse = lax.reduce_precision(x, 8, 7)
    return coarse.astype(jnp.bfloat16), (x - coarse).astype(jnp.bfloat16)


def with_squares(values, squares):
    coarse, fine = halves(squares)
    filler = jnp.zeros((*squares.shape, LANES - 2), jnp.bfloat16)
    return jnp.concatenate(
        [values.astype(jnp.bfloat16), coarse[..., None], fine[..., None], filler], axis=-1
    )


def without_squares(x):
    width = x.shape[-1] - LANES
    tail = x[..., width : width + 2].astype(jnp.float32)
    return x[..., :width], tail[..., 0] + tail[..., 1]


def rotate(queries, position):
    head_size = queries.shape[-1]
    half_dim = head_size // 2
    exponent = jnp.arange(half_dim, dtype=jnp.float32) * (-2.0 / head_size)
    frequency = ROPE_BASE**exponent
    angles = position.astype(jnp.float32)[:, None] * frequency[None, :]
    cosines = jnp.cos(angles)[:, None, :]
    sines = jnp.sin(angles)[:, None, :]
    leading = queries[..., :half_dim]
    trailing = queries[..., half_dim:]
    return jnp.concatenate(
        [leading * cosines - trailing * sines, trailing * cosines + leading * sines], axis=-1
    )


def attend_slots(queries, page_cache, page_table, lengths):
    seq_count, max_pages = page_table.shape
    local_heads, pool_size, page_size, head_size = (
        page_cache.shape[1],
        page_cache.shape[2],
        page_cache.shape[3],
        page_cache.shape[4],
    )
    per_group = queries.shape[1] // local_heads
    used_pages = (lengths + page_size - 1) // page_size
    slot_ids = jnp.arange(pool_size, dtype=jnp.int32)
    page_order = jnp.arange(max_pages, dtype=jnp.int32)
    matches = (page_table[:, :, None] == slot_ids[None, None, :]) & (
        page_order[None, :, None] < used_pages[:, None, None]
    )
    ownership = jnp.any(matches, axis=1)
    page_rank = jnp.sum(jnp.where(matches, page_order[None, :, None], 0), axis=(0, 1))
    length_cap = jnp.sum(jnp.where(ownership, lengths[:, None], 0), axis=0)
    has_owner = jnp.any(ownership, axis=0)
    position = page_rank[:, None] * page_size + jnp.arange(page_size, dtype=jnp.int32)[None, :]
    visible = (position < length_cap[:, None])[None, :, None, :]
    owner_mask = ownership.astype(jnp.bfloat16)
    slot_query = jnp.dot(
        owner_mask.T, queries.reshape(seq_count, -1), preferred_element_type=jnp.float32
    ).astype(jnp.bfloat16)
    slot_query = slot_query.reshape(pool_size, local_heads, per_group, head_size)
    scores = jnp.einsum(
        "phgd,hprd->hpgr", slot_query, page_cache[0], preferred_element_type=jnp.float32
    ) / math.sqrt(head_size)
    scores = jnp.where(visible, scores, -1e30)
    slot_top = jnp.max(scores, axis=3)
    owner_grid = ownership.T[None, :, None, :]
    seq_top = jnp.max(jnp.where(owner_grid, slot_top[..., None], -1e30), axis=1)
    top_slot = jnp.sum(jnp.where(owner_grid, seq_top[:, None, :, :], 0.0), axis=3)
    powers = jnp.where(visible, jnp.exp(scores - top_slot[..., None]), 0.0)
    slot_sum = jnp.sum(powers, axis=3)
    seq_sum = jnp.sum(jnp.where(owner_grid, slot_sum[..., None], 0.0), axis=1)
    sum_slot = jnp.sum(jnp.where(owner_grid, seq_sum[:, None, :, :], 0.0), axis=3)
    divisor = jnp.where(has_owner[None, :, None], sum_slot, 1.0)
    weights = (powers / divisor[..., None]).astype(jnp.bfloat16)
    slot_out = jnp.einsum(
        "hpgr,hprd->phgd", weights, page_cache[1], preferred_element_type=jnp.float32
    )
    result = jnp.dot(
        ownership.astype(jnp.float32),
        slot_out.reshape(pool_size, -1),
        precision=lax.Precision.HIGHEST,
    )
    return result.astype(jnp.bfloat16)


def head_block(place, near, far, near_weight, far_weight, *outs):
    step = pl.program_id(0)
    side = len(outs) // 2
    product = jnp.dot(near[...], near_weight[...], preferred_element_type=jnp.float32)
    product += jnp.dot(far[...], far_weight[...], preferred_element_type=jnp.float32)
    product = product.astype(jnp.bfloat16)
    half = product.shape[0] // 2
    for k in range(side):

        @pl.when(step // side == k)
        def _(k=k):
            outs[k][0] = product[:half]

        @pl.when(step % side == k)
        def _(k=k):
            outs[side + k][0] = product[half:]


def head_partials(near, far, near_weight, far_weight, x_at, y_at, core_at, side, cores):
    rows, depth = near.shape
    width = near_weight.shape[1] // (side * side * cores)
    half = rows // 2

    def weight_block(s, place):
        x_to = (place[0] + s // side) % side
        y_to = (place[1] + s % side) % side
        return (0, (x_to * side + y_to) * cores + place[2])

    out_specs = [
        pl.BlockSpec((1, half, width), lambda s, place, k=k: (jnp.clip(s - side * k, 0, side - 1), 0, 0))
        for k in range(side)
    ] + [
        pl.BlockSpec(
            (1, half, width),
            lambda s, place, k=k: (jnp.clip((s - k + side - 1) // side, 0, side - 1), 0, 0),
        )
        for k in range(side)
    ]
    whole = pl.BlockSpec((rows, depth), lambda s, place: (0, 0))
    weights = pl.BlockSpec((depth, width), weight_block)
    outs = pl.pallas_call(
        head_block,
        grid_spec=pltpu.PrefetchScalarGridSpec(
            num_scalar_prefetch=1,
            grid=(side * side,),
            in_specs=[whole, whole, weights, weights],
            out_specs=out_specs,
        ),
        out_shape=[jax.ShapeDtypeStruct((side, half, width), jnp.bfloat16)] * (2 * side),
        compiler_params=pltpu.CompilerParams(dimension_semantics=("arbitrary",)),
        interpret=INTERPRET,
        name="head_partials",
    )(jnp.stack([x_at, y_at, core_at]).astype(jnp.int32), near, far, near_weight, far_weight)
    return outs[:side], outs[side:]


def summed_along(parts, axis):
    arrived = [shifted(parts[k], axis, k) for k in range(1, len(parts))]
    total = parts[0].astype(jnp.float32)
    for piece in arrived:
        total = total + piece.astype(jnp.float32)
    return total


def joined_all(top, total, axes):
    for axis in axes:
        pieces = sent_to_all(jnp.stack([top, total]), axis)
        tops = pieces[:, 0]
        top = jnp.max(tops, axis=0)
        total = jnp.sum(pieces[:, 1] * jnp.exp(tops - top[None]), axis=0)
    return top, total


def local(
    stream,
    input_gain,
    query_bias,
    query_weight,
    out_weight,
    page_cache,
    page_table,
    lengths,
    final_gain,
    head_weight,
):
    side, cores, batches = lax.axis_size("mp_0"), lax.axis_size("mp_2"), lax.axis_size("batch")
    members = side * side * cores
    x_at, y_at, core_at = lax.axis_index("mp_0"), lax.axis_index("mp_1"), lax.axis_index("mp_2")
    batch_at = lax.axis_index("batch")
    first_core = core_at == 0
    seqs, features_here = stream.shape
    full_width = features_here * members
    seq_count = page_table.shape[0]
    head_size = page_cache.shape[-1]

    far_head_weight = shifted(head_weight, "mp_2", 1)
    far_out_weight = shifted(out_weight, "mp_2", 1)

    features = stream.astype(jnp.float32)
    scaled = (features * input_gain).astype(jnp.bfloat16)
    products = jnp.dot(scaled, query_weight, preferred_element_type=jnp.float32)
    payload = with_squares(products, jnp.sum(features * features, axis=1))
    arrived = lax.all_to_all(
        payload.reshape(members, seq_count, -1), MP, split_axis=0, concat_axis=0, tiled=True
    )
    products, squares = without_squares(arrived)
    scale = lax.rsqrt(jnp.sum(squares, axis=0) / full_width + EPS)
    queries = jnp.sum(products.astype(jnp.float32), axis=0) * scale[:, None] + query_bias
    queries = rotate(queries.reshape(seq_count, -1, head_size), lengths - 1).astype(jnp.bfloat16)
    attended = attend_slots(queries, page_cache, page_table, lengths)

    mine = sent_to_all(attended, XY).reshape(side * side * seq_count, -1)
    near_out = jnp.dot(mine, out_weight, preferred_element_type=jnp.float32)
    far_out = jnp.dot(mine, far_out_weight, preferred_element_type=jnp.float32)
    partial_out = jnp.concatenate(
        [jnp.where(first_core, near_out, far_out), jnp.where(first_core, far_out, near_out)], axis=1
    ).astype(jnp.bfloat16)
    per_batch = side * side // batches
    arrived = lax.all_to_all(
        partial_out.reshape(batches, per_batch * seq_count, -1),
        "batch",
        split_axis=0,
        concat_axis=0,
        tiled=True,
    )
    rows = stream.reshape(batches, per_batch, cores, seq_count, features_here)
    rows = lax.dynamic_index_in_dim(rows, batch_at, 0, keepdims=False)

    def of_core(core):
        taken = lax.dynamic_index_in_dim(rows, core, 1, keepdims=False).reshape(-1, features_here)
        return jnp.concatenate([taken.astype(jnp.float32), final_gain[None]], axis=0)

    near_rows = of_core(core_at)
    far_rows = shifted(of_core(1 - core_at), "mp_2", 1)
    both = jnp.concatenate(
        [jnp.where(first_core, near_rows, far_rows), jnp.where(first_core, far_rows, near_rows)],
        axis=1,
    )
    residual = both[:-1] + jnp.sum(arrived.astype(jnp.float32), axis=0)
    payload = with_squares(residual * both[-1:], jnp.sum(residual * residual, axis=1))
    gathered = sent_to_all(payload, BATCH_CORE).reshape(batches, cores, per_batch, seq_count, -1)
    gathered = jnp.moveaxis(gathered, 1, 2).reshape(seqs, -1)
    scaled_out, squares_here = without_squares(gathered)
    near = jnp.where(first_core, scaled_out[:, :features_here], scaled_out[:, features_here:])
    far = jnp.where(first_core, scaled_out[:, features_here:], scaled_out[:, :features_here])
    upper, lower = head_partials(
        near, far, head_weight, far_head_weight, x_at, y_at, core_at, side, cores
    )
    squares_out = jnp.sum(sent_to_all(squares_here, XY), axis=0)
    scale_out = lax.rsqrt(squares_out / full_width + EPS)
    upper = summed_along(upper, "mp_0").astype(jnp.bfloat16)
    lower = summed_along(lower, "mp_1").astype(jnp.bfloat16)
    upper = summed_along([upper[k] for k in range(side)], "mp_1")
    lower = summed_along([lower[k] for k in range(side)], "mp_0")
    logits = jnp.concatenate([upper, lower], axis=0) * scale_out[:, None]

    local_top = jnp.max(logits, axis=1)
    local_sum = jnp.sum(jnp.exp(logits - local_top[:, None]), axis=1)
    highest, summed = joined_all(local_top, local_sum, (MP, "batch"))
    return (logits, jnp.log(summed) + highest)


def solution(mesh):
    torus = Mesh(
        mesh.devices.reshape(mesh.shape["batch"], 4, 4, 2), ("batch", "mp_0", "mp_1", "mp_2")
    )
    in_specs = (
        P(None, MP),
        P(MP),
        P("batch"),
        P(MP, "batch"),
        P("batch", MP),
        P(None, "batch", MP, None, None),
        P(MP, None),
        P(MP),
        P(MP),
        P(MP, "batch"),
    )
    out_specs = (P(None, BATCH_MP), P())
    return jax.shard_map(local, mesh=torus, in_specs=in_specs, out_specs=out_specs, check_vma=False)
```

```python
import math

import jax
import jax.numpy as jnp
from jax import lax
from jax.experimental import pallas as pl
from jax.experimental.pallas import tpu as pltpu
from jax.sharding import Mesh
from jax.sharding import PartitionSpec as P

MP = ("mp_0", "mp_1", "mp_2")
BATCH_MP = ("batch", "mp_0", "mp_1", "mp_2")
XY = ("mp_0", "mp_1")
BATCH_CORE = ("batch", "mp_2")


EPS = 1e-06
ROPE_BASE = 1000000.0
INTERPRET = False

LANES = 128


def sent_to_all(x, axis):
    length = lax.axis_size(axis)
    return lax.all_to_all(jnp.broadcast_to(x[None], (length, *x.shape)), axis, 0, 0, tiled=True)


def shifted(x, axis, by):
    length = lax.axis_size(axis)
    return lax.ppermute(x, axis, [(k, (k + by) % length) for k in range(length)])


def halves(x):
    coarse = lax.reduce_precision(x, 8, 7)
    return coarse.astype(jnp.bfloat16), (x - coarse).astype(jnp.bfloat16)


def with_squares(values, squares):
    coarse, fine = halves(squares)
    filler = jnp.zeros((*squares.shape, LANES - 2), jnp.bfloat16)
    return jnp.concatenate(
        [values.astype(jnp.bfloat16), coarse[..., None], fine[..., None], filler], axis=-1
    )


def without_squares(x):
    width = x.shape[-1] - LANES
    tail = x[..., width : width + 2].astype(jnp.float32)
    return x[..., :width], tail[..., 0] + tail[..., 1]


def rotate(queries, position):
    head_size = queries.shape[-1]
    half_dim = head_size // 2
    exponent = jnp.arange(half_dim, dtype=jnp.float32) * (-2.0 / head_size)
    frequency = ROPE_BASE**exponent
    angles = position.astype(jnp.float32)[:, None] * frequency[None, :]
    cosines = jnp.cos(angles)[:, None, :]
    sines = jnp.sin(angles)[:, None, :]
    leading = queries[..., :half_dim]
    trailing = queries[..., half_dim:]
    return jnp.concatenate(
        [leading * cosines - trailing * sines, trailing * cosines + leading * sines], axis=-1
    )


def attend_slots(queries, page_cache, page_table, lengths):
    seq_count, max_pages = page_table.shape
    local_heads, pool_size, page_size, head_size = (
        page_cache.shape[1],
        page_cache.shape[2],
        page_cache.shape[3],
        page_cache.shape[4],
    )
    per_group = queries.shape[1] // local_heads
    used_pages = (lengths + page_size - 1) // page_size
    slot_ids = jnp.arange(pool_size, dtype=jnp.int32)
    page_order = jnp.arange(max_pages, dtype=jnp.int32)
    matches = (page_table[:, :, None] == slot_ids[None, None, :]) & (
        page_order[None, :, None] < used_pages[:, None, None]
    )
    ownership = jnp.any(matches, axis=1)
    page_rank = jnp.sum(jnp.where(matches, page_order[None, :, None], 0), axis=(0, 1))
    length_cap = jnp.sum(jnp.where(ownership, lengths[:, None], 0), axis=0)
    has_owner = jnp.any(ownership, axis=0)
    position = page_rank[:, None] * page_size + jnp.arange(page_size, dtype=jnp.int32)[None, :]
    visible = (position < length_cap[:, None])[None, :, None, :]
    owner_mask = ownership.astype(jnp.bfloat16)
    slot_query = jnp.dot(
        owner_mask.T, queries.reshape(seq_count, -1), preferred_element_type=jnp.float32
    ).astype(jnp.bfloat16)
    slot_query = slot_query.reshape(pool_size, local_heads, per_group, head_size)
    scores = jnp.einsum(
        "phgd,hprd->hpgr", slot_query, page_cache[0], preferred_element_type=jnp.float32
    ) / math.sqrt(head_size)
    scores = jnp.where(visible, scores, -1e30)
    slot_top = jnp.max(scores, axis=3)
    owner_grid = ownership.T[None, :, None, :]
    seq_top = jnp.max(jnp.where(owner_grid, slot_top[..., None], -1e30), axis=1)
    top_slot = jnp.sum(jnp.where(owner_grid, seq_top[:, None, :, :], 0.0), axis=3)
    powers = jnp.where(visible, jnp.exp(scores - top_slot[..., None]), 0.0)
    slot_sum = jnp.sum(powers, axis=3)
    seq_sum = jnp.sum(jnp.where(owner_grid, slot_sum[..., None], 0.0), axis=1)
    sum_slot = jnp.sum(jnp.where(owner_grid, seq_sum[:, None, :, :], 0.0), axis=3)
    divisor = jnp.where(has_owner[None, :, None], sum_slot, 1.0)
    weights = (powers / divisor[..., None]).astype(jnp.bfloat16)
    slot_out = jnp.einsum(
        "hpgr,hprd->phgd", weights, page_cache[1], preferred_element_type=jnp.float32
    )
    result = jnp.dot(
        ownership.astype(jnp.float32),
        slot_out.reshape(pool_size, -1),
        precision=lax.Precision.HIGHEST,
    )
    return result.astype(jnp.bfloat16)


def head_block(place, near, far, *refs):
    side = len(refs) // 4
    near_weights, far_weights = refs[:side], refs[side : 2 * side]
    by_x, by_y = refs[2 * side : 3 * side], refs[3 * side :]
    step = pl.program_id(0)
    half = near.shape[0] // 2
    for k in range(side):
        product = jnp.dot(near[...], near_weights[k][...], preferred_element_type=jnp.float32)
        product += jnp.dot(far[...], far_weights[k][...], preferred_element_type=jnp.float32)
        product = product.astype(jnp.bfloat16)
        by_y[k][0] = product[half:]
        for x_step in range(side):

            @pl.when(step == x_step)
            def _(k=k, x_step=x_step, product=product):
                by_x[x_step][k] = product[:half]


def head_partials(near, far, near_weight, far_weight, x_at, y_at, core_at, side, cores):
    rows, depth = near.shape
    width = near_weight.shape[1] // (side * side * cores)
    half = rows // 2

    def weight_block(k):
        def at(s, place):
            x_to = (place[0] + s) % side
            y_to = (place[1] + k) % side
            return (0, (x_to * side + y_to) * cores + place[2])

        return pl.BlockSpec((depth, width), at)

    out_specs = [pl.BlockSpec((side, half, width), lambda s, place: (0, 0, 0))] * side
    out_specs += [pl.BlockSpec((1, half, width), lambda s, place: (s, 0, 0))] * side
    whole = pl.BlockSpec((rows, depth), lambda s, place: (0, 0))
    weights = [weight_block(k) for k in range(side)]
    outs = pl.pallas_call(
        head_block,
        grid_spec=pltpu.PrefetchScalarGridSpec(
            num_scalar_prefetch=1,
            grid=(side,),
            in_specs=[whole, whole, *weights, *weights],
            out_specs=out_specs,
        ),
        out_shape=[jax.ShapeDtypeStruct((side, half, width), jnp.bfloat16)] * (2 * side),
        compiler_params=pltpu.CompilerParams(dimension_semantics=("arbitrary",)),
        interpret=INTERPRET,
        name="head_partials",
    )(
        jnp.stack([x_at, y_at, core_at]).astype(jnp.int32),
        near,
        far,
        *[near_weight] * side,
        *[far_weight] * side,
    )
    return outs[:side], outs[side:]


def summed_along(parts, axis):
    arrived = [shifted(parts[k], axis, k) for k in range(1, len(parts))]
    total = parts[0].astype(jnp.float32)
    for piece in arrived:
        total = total + piece.astype(jnp.float32)
    return total


def joined_all(top, total, axes):
    for axis in axes:
        pieces = sent_to_all(jnp.stack([top, total]), axis)
        tops = pieces[:, 0]
        top = jnp.max(tops, axis=0)
        total = jnp.sum(pieces[:, 1] * jnp.exp(tops - top[None]), axis=0)
    return top, total


def local(
    stream,
    input_gain,
    query_bias,
    query_weight,
    out_weight,
    page_cache,
    page_table,
    lengths,
    final_gain,
    head_weight,
):
    side, cores, batches = lax.axis_size("mp_0"), lax.axis_size("mp_2"), lax.axis_size("batch")
    members = side * side * cores
    x_at, y_at, core_at = lax.axis_index("mp_0"), lax.axis_index("mp_1"), lax.axis_index("mp_2")
    batch_at = lax.axis_index("batch")
    first_core = core_at == 0
    seqs, features_here = stream.shape
    full_width = features_here * members
    seq_count = page_table.shape[0]
    head_size = page_cache.shape[-1]

    far_head_weight = shifted(head_weight, "mp_2", 1)
    far_out_weight = shifted(out_weight, "mp_2", 1)

    features = stream.astype(jnp.float32)
    scaled = (features * input_gain).astype(jnp.bfloat16)
    products = jnp.dot(scaled, query_weight, preferred_element_type=jnp.float32)
    payload = with_squares(products, jnp.sum(features * features, axis=1))
    arrived = lax.all_to_all(
        payload.reshape(members, seq_count, -1), MP, split_axis=0, concat_axis=0, tiled=True
    )
    products, squares = without_squares(arrived)
    scale = lax.rsqrt(jnp.sum(squares, axis=0) / full_width + EPS)
    queries = jnp.sum(products.astype(jnp.float32), axis=0) * scale[:, None] + query_bias
    queries = rotate(queries.reshape(seq_count, -1, head_size), lengths - 1).astype(jnp.bfloat16)
    attended = attend_slots(queries, page_cache, page_table, lengths)

    mine = sent_to_all(attended, XY).reshape(side * side * seq_count, -1)
    near_out = jnp.dot(mine, out_weight, preferred_element_type=jnp.float32)
    far_out = jnp.dot(mine, far_out_weight, preferred_element_type=jnp.float32)
    partial_out = jnp.concatenate(
        [jnp.where(first_core, near_out, far_out), jnp.where(first_core, far_out, near_out)], axis=1
    ).astype(jnp.bfloat16)
    per_batch = side * side // batches
    arrived = lax.all_to_all(
        partial_out.reshape(batches, per_batch * seq_count, -1),
        "batch",
        split_axis=0,
        concat_axis=0,
        tiled=True,
    )
    rows = stream.reshape(batches, per_batch, cores, seq_count, features_here)
    rows = lax.dynamic_index_in_dim(rows, batch_at, 0, keepdims=False)

    def of_core(core):
        taken = lax.dynamic_index_in_dim(rows, core, 1, keepdims=False).reshape(-1, features_here)
        return jnp.concatenate([taken.astype(jnp.float32), final_gain[None]], axis=0)

    near_rows = of_core(core_at)
    far_rows = shifted(of_core(1 - core_at), "mp_2", 1)
    both = jnp.concatenate(
        [jnp.where(first_core, near_rows, far_rows), jnp.where(first_core, far_rows, near_rows)],
        axis=1,
    )
    residual = both[:-1] + jnp.sum(arrived.astype(jnp.float32), axis=0)
    payload = (residual * both[-1:]).astype(jnp.bfloat16)
    gathered = sent_to_all(payload, BATCH_CORE).reshape(batches, cores, per_batch, seq_count, -1)
    scaled_out = jnp.moveaxis(gathered, 1, 2).reshape(seqs, -1)
    unscaled = scaled_out.astype(jnp.float32) / both[-1:]
    squares_here = jnp.sum(unscaled * unscaled, axis=1)
    squares_out = summed_along([squares_here] * side, "mp_0")
    near = jnp.where(first_core, scaled_out[:, :features_here], scaled_out[:, features_here:])
    far = jnp.where(first_core, scaled_out[:, features_here:], scaled_out[:, :features_here])
    upper, lower = head_partials(
        near, far, head_weight, far_head_weight, x_at, y_at, core_at, side, cores
    )
    squares_out = summed_along([squares_out] * side, "mp_1")
    scale_out = lax.rsqrt(squares_out / full_width + EPS)
    upper = summed_along(upper, "mp_0").astype(jnp.bfloat16)
    lower = summed_along(lower, "mp_1").astype(jnp.bfloat16)
    upper = summed_along([upper[k] for k in range(side)], "mp_1")
    lower = summed_along([lower[k] for k in range(side)], "mp_0")
    logits = jnp.concatenate([upper, lower], axis=0) * scale_out[:, None]

    local_top = jnp.max(logits, axis=1)
    local_sum = jnp.sum(jnp.exp(logits - local_top[:, None]), axis=1)
    highest, summed = joined_all(local_top, local_sum, (BATCH_MP,))
    return (logits, jnp.log(summed) + highest)


def solution(mesh):
    torus = Mesh(
        mesh.devices.reshape(mesh.shape["batch"], 4, 4, 2), ("batch", "mp_0", "mp_1", "mp_2")
    )
    in_specs = (
        P(None, MP),
        P(MP),
        P("batch"),
        P(MP, "batch"),
        P("batch", MP),
        P(None, "batch", MP, None, None),
        P(MP, None),
        P(MP),
        P(MP),
        P(MP, "batch"),
    )
    out_specs = (P(None, BATCH_MP), P())

    def step(*args):
        return local(*args)

    step = jax.shard_map(step, mesh=torus, in_specs=in_specs, out_specs=out_specs, check_vma=False)
    return step
```

```python
import functools
import math

import jax
import jax.numpy as jnp
from jax import lax
from jax.experimental import pallas as pl
from jax.experimental.pallas import tpu as pltpu
from jax.sharding import Mesh
from jax.sharding import PartitionSpec as P

MP = ("mp_0", "mp_1", "mp_2")
BATCH_MP = ("batch", "mp_0", "mp_1", "mp_2")
XY = ("mp_0", "mp_1")
BATCH_CORE = ("batch", "mp_2")


EPS = 1e-06
ROPE_BASE = 1000000.0
INTERPRET = False

LANES = 128


def sent_to_all(x, axis):
    length = lax.axis_size(axis)
    return lax.all_to_all(jnp.broadcast_to(x[None], (length, *x.shape)), axis, 0, 0, tiled=True)


def shifted(x, axis, by):
    length = lax.axis_size(axis)
    return lax.ppermute(x, axis, [(k, (k + by) % length) for k in range(length)])


def query_block(stream, gain, weight, out):
    width = weight.shape[1]
    features = stream[...].astype(jnp.float32)
    squares = jnp.sum(features * features, axis=1, keepdims=True)
    products = jnp.dot(
        (features * gain[...]).astype(jnp.bfloat16), weight[...], preferred_element_type=jnp.float32
    )
    out[:, :width] = products.astype(jnp.bfloat16)
    coarse = squares.astype(jnp.bfloat16).astype(jnp.float32)
    lane = lax.broadcasted_iota(jnp.int32, (features.shape[0], LANES), 1)
    tail = jnp.where(lane == 0, coarse, jnp.where(lane == 1, squares - coarse, 0.0))
    out[:, width:] = tail.astype(jnp.bfloat16)


def query_parts(stream, gain, weight):
    return pl.pallas_call(
        query_block,
        out_shape=jax.ShapeDtypeStruct((stream.shape[0], weight.shape[1] + LANES), jnp.bfloat16),
        interpret=INTERPRET,
        name="query_parts",
    )(stream, gain[None], weight)


def turns(position, head_size):
    half_dim = head_size // 2
    exponent = jnp.arange(half_dim, dtype=jnp.float32) * (-2.0 / head_size)
    frequency = ROPE_BASE**exponent
    angles = position.astype(jnp.float32)[:, None] * frequency[None, :]
    cosines, sines = jnp.cos(angles), jnp.sin(angles)
    return (
        jnp.concatenate([cosines, cosines], axis=1),
        jnp.concatenate([-sines, sines], axis=1),
    )


def token_owners(page_table, lengths, pool_size, page_size):
    seq_count, max_pages = page_table.shape
    page_order = jnp.arange(max_pages, dtype=jnp.int32)
    used_pages = (lengths + page_size - 1) // page_size
    slot_ids = jnp.arange(pool_size, dtype=jnp.int32)
    matches = (page_table[:, :, None] == slot_ids[None, None, :]) & (
        page_order[None, :, None] < used_pages[:, None, None]
    )
    seq_ids = jnp.arange(seq_count, dtype=jnp.int32)
    owner = jnp.sum(jnp.where(matches, seq_ids[:, None, None], 0), axis=(0, 1))
    remaining = lengths[:, None] - page_order[None, :] * page_size
    visible = jnp.sum(jnp.where(matches, remaining[:, :, None], 0), axis=(0, 1))
    at = jnp.arange(page_size, dtype=jnp.int32)
    return jnp.where(at[None, :] < visible[:, None], owner[:, None], -1)


def attend_block(full_width, sums, bias, cosines, sines, owners, pages, out, *scratch):
    keys, values, scores, sems = scratch
    copies, seq_count, width = out.shape
    pool_size, page_size, head_size = keys.shape
    heads = width // head_size
    rows = heads * seq_count
    chunks = sems.shape[1]
    slots = pool_size // chunks
    tokens = slots * page_size

    fetches = []
    for kind, held in enumerate((keys, values)):
        for k in range(chunks):
            at = pl.ds(k * slots, slots)
            copy = pltpu.make_async_copy(pages.at[kind, 0, at], held.at[at], sems.at[kind, k])
            copy.start()
            fetches.append(copy)

    tail = sums[:, width:]
    lane = lax.broadcasted_iota(jnp.int32, tail.shape, 1)
    squares = jnp.sum(jnp.where(lane < 2, tail, 0.0), axis=1, keepdims=True)
    turned = sums[:, :width] * lax.rsqrt(squares / full_width + EPS) + bias[...]
    pieces = []
    for k in range(heads):
        piece = turned[:, k * head_size : (k + 1) * head_size]
        across = pltpu.roll(piece, head_size // 2, 1)
        pieces.append(piece * cosines[...] + across * sines[...])
    queries = jnp.concatenate(pieces, axis=0).astype(jnp.bfloat16)

    row_seq = lax.broadcasted_iota(jnp.int32, (rows, 1), 0) % seq_count
    highest = jnp.full((rows, head_size), -1e30, jnp.float32)
    for k in range(chunks):
        fetches[k].wait()
        key = keys[k * slots : (k + 1) * slots].reshape(tokens, head_size)
        here = lax.dot_general(
            queries, key, (((1,), (1,)), ((), ())), preferred_element_type=jnp.float32
        ) * (1.0 / math.sqrt(head_size))
        at = slice(k * tokens, (k + 1) * tokens)
        here = jnp.where(owners[:, at] == row_seq, here, -1e30)
        scores[:, at] = here
        for t in range(tokens // head_size):
            highest = jnp.maximum(highest, here[:, t * head_size : (t + 1) * head_size])
    highest = jnp.max(highest, axis=1, keepdims=True)
    summed = jnp.zeros((rows, head_size), jnp.float32)
    mixed = jnp.zeros((rows, head_size), jnp.float32)
    for k in range(chunks):
        powers = jnp.exp(scores[:, k * tokens : (k + 1) * tokens] - highest)
        for t in range(tokens // head_size):
            summed += powers[:, t * head_size : (t + 1) * head_size]
        fetches[chunks + k].wait()
        value = values[k * slots : (k + 1) * slots].reshape(tokens, head_size)
        mixed += jnp.dot(powers.astype(jnp.bfloat16), value, preferred_element_type=jnp.float32)
    result = mixed / jnp.sum(summed, axis=1, keepdims=True)
    row = [result[k * seq_count : (k + 1) * seq_count] for k in range(heads)]
    row = jnp.concatenate(row, axis=1).astype(jnp.bfloat16)
    for k in range(copies):
        out[k] = row


def attend(sums, bias, cosines, sines, owners, page_cache, full_width, copies, chunks=8):
    seq_count, width = sums.shape
    width -= LANES
    pool_size, page_size, head_size = page_cache.shape[2:]
    pool = (pool_size, page_size, head_size)
    rows = width // head_size * seq_count
    in_hbm = pl.BlockSpec(memory_space=pltpu.HBM)
    in_vmem = pl.BlockSpec(memory_space=pltpu.VMEM)
    return pl.pallas_call(
        functools.partial(attend_block, full_width),
        in_specs=[in_vmem, in_vmem, in_vmem, in_vmem, in_vmem, in_hbm],
        out_specs=in_vmem,
        out_shape=jax.ShapeDtypeStruct((copies, seq_count, width), jnp.bfloat16),
        scratch_shapes=[
            pltpu.VMEM(pool, jnp.bfloat16),
            pltpu.VMEM(pool, jnp.bfloat16),
            pltpu.VMEM((rows, pool_size * page_size), jnp.float32),
            pltpu.SemaphoreType.DMA((2, chunks)),
        ],
        interpret=INTERPRET,
        name="attend",
    )(sums, bias[None], cosines, sines, owners.reshape(1, -1), page_cache)


def head_block(place, gain, gathered_far, near_weight, far_weight, *refs):
    batches, cores, per_batch, _, depth = gathered_far.shape
    side = (len(refs) - 7) // 2
    out_x, out_y = refs[:side], refs[side : 2 * side]
    gathered, weights, block_x, block_y, sem, sems_in, sems_out = refs[2 * side :]
    fetch = pltpu.make_async_copy(gathered_far, gathered, sem)
    fetch.start()
    x_at, y_at, core_at = place[0], place[1], place[2]
    width = near_weight.shape[1] // (side * side * cores)
    rows_here = depth // cores

    def weight_copies(x_to, y_to):
        column = (((x_at + x_to) % side) * side + (y_at + y_to) % side) * cores + core_at
        column = pl.multiple_of(column * width, width)
        copies = []
        for k, (weight, core) in enumerate(((near_weight, core_at), (far_weight, 1 - core_at))):
            row = pl.multiple_of(core * rows_here, rows_here)
            copies.append(
                pltpu.make_async_copy(
                    weight.at[:, pl.ds(column, width)],
                    weights.at[x_to, pl.ds(row, rows_here), pl.ds(y_to * width, width)],
                    sems_in.at[x_to, y_to * 2 + k],
                )
            )
        return copies

    loads = [[c for y_to in range(side) for c in weight_copies(x_to, y_to)] for x_to in range(side)]
    for copies in loads:
        for copy in copies:
            copy.start()

    fetch.wait()
    pieces = [
        gathered[b, c, i].astype(jnp.float32)
        for b in range(batches)
        for i in range(per_batch)
        for c in range(cores)
    ]
    ordered = jnp.concatenate(pieces, axis=0)
    features = ordered.astype(jnp.bfloat16)
    half = ordered.shape[0] // 2
    unscaled = ordered / gain[...]
    extra = block_x.shape[2] - half
    squares = lax.dot_general(
        jnp.ones((extra, depth), jnp.float32),
        unscaled * unscaled,
        (((1,), (1,)), ((), ())),
        precision=lax.Precision.HIGHEST,
        preferred_element_type=jnp.float32,
    )
    coarse = squares.astype(jnp.bfloat16)
    fine = (squares - coarse.astype(jnp.float32)).astype(jnp.bfloat16)
    filler = jnp.zeros((extra, width - 2 * half), jnp.bfloat16)
    tail_x = jnp.concatenate([coarse[:, :half], fine[:, :half], filler], axis=1)
    tail_y = jnp.concatenate([coarse[:, half:], fine[:, half:], filler], axis=1)

    stores = []
    for x_to in range(side):
        for copy in loads[x_to]:
            copy.wait()
        product = jnp.dot(features, weights[x_to], preferred_element_type=jnp.float32)
        for y_to in range(side):
            part = product[:, y_to * width : (y_to + 1) * width].astype(jnp.bfloat16)
            block_x[x_to, y_to, :half] = part[:half]
            block_x[x_to, y_to, half:] = tail_x
            block_y[y_to, x_to, :half] = part[half:]
            block_y[y_to, x_to, half:] = tail_y
            for copy in (
                pltpu.make_async_copy(
                    block_x.at[x_to, y_to], out_x[x_to].at[y_to], sems_out.at[0, x_to, y_to]
                ),
                pltpu.make_async_copy(
                    block_y.at[y_to, x_to], out_y[y_to].at[x_to], sems_out.at[1, x_to, y_to]
                ),
            ):
                copy.start()
                stores.append(copy)
    for copy in stores:
        copy.wait()


def head_partials(gathered, gain, near_weight, far_weight, x_at, y_at, core_at, side):
    batches, cores, per_batch, seq_count, depth = gathered.shape
    half = batches * cores * per_batch * seq_count // 2
    width = near_weight.shape[1] // (side * side * cores)
    block = (side, half + 8, width)
    in_hbm = pl.BlockSpec(memory_space=pltpu.HBM)
    outs = pl.pallas_call(
        head_block,
        in_specs=[
            pl.BlockSpec(memory_space=pltpu.SMEM),
            pl.BlockSpec(memory_space=pltpu.VMEM),
            in_hbm,
            in_hbm,
            in_hbm,
        ],
        out_specs=[in_hbm] * (2 * side),
        out_shape=[jax.ShapeDtypeStruct(block, jnp.bfloat16)] * (2 * side),
        scratch_shapes=[
            pltpu.VMEM(gathered.shape, jnp.bfloat16),
            pltpu.VMEM((side, depth, side * width), jnp.bfloat16),
            pltpu.VMEM((side, *block), jnp.bfloat16),
            pltpu.VMEM((side, *block), jnp.bfloat16),
            pltpu.SemaphoreType.DMA,
            pltpu.SemaphoreType.DMA((side, 2 * side)),
            pltpu.SemaphoreType.DMA((2, side, side)),
        ],
        interpret=INTERPRET,
        name="head_partials",
    )(
        jnp.stack([x_at, y_at, core_at]).astype(jnp.int32),
        gain,
        gathered,
        near_weight,
        far_weight,
    )
    return outs[:side], outs[side:]


def summed_along(parts, axis):
    arrived = [shifted(parts[k], axis, k) for k in range(1, len(parts))]
    total = parts[0].astype(jnp.float32)
    for piece in arrived:
        total = total + piece.astype(jnp.float32)
    return total


def joined_all(top, total, axes):
    for axis in axes:
        pieces = sent_to_all(jnp.stack([top, total]), axis)
        tops = pieces[:, 0]
        top = jnp.max(tops, axis=0)
        total = jnp.sum(pieces[:, 1] * jnp.exp(tops - top[None]), axis=0)
    return top, total


def local(
    stream,
    input_gain,
    query_bias,
    query_weight,
    out_weight,
    page_cache,
    page_table,
    lengths,
    final_gain,
    head_weight,
):
    side, cores, batches = lax.axis_size("mp_0"), lax.axis_size("mp_2"), lax.axis_size("batch")
    members = side * side * cores
    x_at, y_at, core_at = lax.axis_index("mp_0"), lax.axis_index("mp_1"), lax.axis_index("mp_2")
    batch_at = lax.axis_index("batch")
    first_core = core_at == 0
    seqs, features_here = stream.shape
    full_width = features_here * members
    seq_count = page_table.shape[0]
    head_size = page_cache.shape[-1]

    far_head_weight = shifted(head_weight, "mp_2", 1)
    far_out_weight = shifted(out_weight, "mp_2", 1)

    parts = query_parts(stream, input_gain, query_weight).reshape(members, seq_count, -1)
    parts = lax.all_to_all(parts, MP, split_axis=0, concat_axis=0, tiled=True)
    owners = token_owners(page_table, lengths, *page_cache.shape[2:4])
    cosines, sines = turns(lengths - 1, head_size)
    sums = jnp.sum(parts.astype(jnp.float32), axis=0)
    attended = attend(
        sums, query_bias, cosines, sines, owners, page_cache, full_width, side * side
    )

    mine = lax.all_to_all(attended, XY, 0, 0, tiled=True).reshape(side * side * seq_count, -1)
    both_out = jnp.concatenate(
        [
            jnp.where(first_core, out_weight, far_out_weight),
            jnp.where(first_core, far_out_weight, out_weight),
        ],
        axis=1,
    )
    both_out = lax.optimization_barrier(both_out)
    partial_out = jnp.dot(mine, both_out, preferred_element_type=jnp.float32).astype(jnp.bfloat16)
    per_batch = side * side // batches
    arrived = lax.all_to_all(
        partial_out.reshape(batches, per_batch * seq_count, -1),
        "batch",
        split_axis=0,
        concat_axis=0,
        tiled=True,
    )
    rows = stream.reshape(batches, per_batch, cores, seq_count, features_here)
    rows = lax.dynamic_index_in_dim(rows, batch_at, 0, keepdims=False)

    def of_core(core):
        taken = lax.dynamic_index_in_dim(rows, core, 1, keepdims=False).reshape(-1, features_here)
        return jnp.concatenate([taken.astype(jnp.float32), final_gain[None]], axis=0)

    near_rows = of_core(core_at)
    far_rows = shifted(of_core(1 - core_at), "mp_2", 1)
    both = jnp.concatenate(
        [jnp.where(first_core, near_rows, far_rows), jnp.where(first_core, far_rows, near_rows)],
        axis=1,
    )
    residual = both[:-1] + jnp.sum(arrived.astype(jnp.float32), axis=0)
    payload = (residual * both[-1:]).astype(jnp.bfloat16)
    gathered = sent_to_all(payload, BATCH_CORE).reshape(batches, cores, per_batch, seq_count, -1)
    upper, lower = head_partials(
        gathered, both[-1:], head_weight, far_head_weight, x_at, y_at, core_at, side
    )
    upper = summed_along(upper, "mp_0").astype(jnp.bfloat16)
    lower = summed_along(lower, "mp_1").astype(jnp.bfloat16)
    upper = summed_along([upper[k] for k in range(side)], "mp_1")
    lower = summed_along([lower[k] for k in range(side)], "mp_0")

    def rescaled(total):
        half = seqs // 2
        squares = total[half, :half] + total[half, half : 2 * half]
        return total[:half] * lax.rsqrt(squares / full_width + EPS)[:, None]

    logits = jnp.concatenate([rescaled(upper), rescaled(lower)], axis=0)

    local_top = jnp.max(logits, axis=1)
    local_sum = jnp.sum(jnp.exp(logits - local_top[:, None]), axis=1)
    highest, summed = joined_all(local_top, local_sum, (MP, "batch"))
    return (logits, jnp.log(summed) + highest)


def solution(mesh):
    torus = Mesh(
        mesh.devices.reshape(mesh.shape["batch"], 4, 4, 2), ("batch", "mp_0", "mp_1", "mp_2")
    )
    in_specs = (
        P(None, MP),
        P(MP),
        P("batch"),
        P(MP, "batch"),
        P("batch", MP),
        P(None, "batch", MP, None, None),
        P(MP, None),
        P(MP),
        P(MP),
        P(MP, "batch"),
    )
    out_specs = (P(None, BATCH_MP), P())

    def step(*args):
        return local(*args)

    step = jax.shard_map(step, mesh=torus, in_specs=in_specs, out_specs=out_specs, check_vma=False)
    return step
```

```python
import functools
import math

import jax
import jax.numpy as jnp
from jax import lax
from jax.experimental import pallas as pl
from jax.experimental.pallas import tpu as pltpu
from jax.sharding import Mesh
from jax.sharding import PartitionSpec as P

MP = ("mp_0", "mp_1", "mp_2")
BATCH_MP = ("batch", "mp_0", "mp_1", "mp_2")
XY = ("mp_0", "mp_1")
BATCH_CORE = ("batch", "mp_2")


EPS = 1e-06
ROPE_BASE = 1000000.0
INTERPRET = False

LANES = 128
HEAD_VMEM = 24 * 2**20
ATTEND_VMEM = 16 * 2**20


def near_by(x):
    return pltpu.with_memory_space_constraint(x, pltpu.VMEM)


def far_off(x):
    return pltpu.with_memory_space_constraint(x, pltpu.HBM)


def sent_to_all(x, axis):
    length = lax.axis_size(axis)
    return lax.all_to_all(jnp.broadcast_to(x[None], (length, *x.shape)), axis, 0, 0, tiled=True)


def shifted(x, axis, by):
    length = lax.axis_size(axis)
    return lax.ppermute(x, axis, [(k, (k + by) % length) for k in range(length)])


def query_block(stream, gain, weight, out):
    width = weight.shape[1]
    features = stream[...].astype(jnp.float32)
    squares = jnp.sum(features * features, axis=1, keepdims=True)
    products = jnp.dot(
        (features * gain[...]).astype(jnp.bfloat16), weight[...], preferred_element_type=jnp.float32
    )
    out[:, :width] = products.astype(jnp.bfloat16)
    coarse = squares.astype(jnp.bfloat16).astype(jnp.float32)
    lane = lax.broadcasted_iota(jnp.int32, (features.shape[0], LANES), 1)
    tail = jnp.where(lane == 0, coarse, jnp.where(lane == 1, squares - coarse, 0.0))
    out[:, width:] = tail.astype(jnp.bfloat16)


def query_parts(stream, gain, weight):
    return pl.pallas_call(
        query_block,
        out_shape=pltpu.VMEM((stream.shape[0], weight.shape[1] + LANES), jnp.bfloat16),
        interpret=INTERPRET,
        name="query_parts",
    )(stream, gain[None], weight)


def turns(position, head_size):
    half_dim = head_size // 2
    exponent = jnp.arange(half_dim, dtype=jnp.float32) * (-2.0 / head_size)
    frequency = ROPE_BASE**exponent
    angles = position.astype(jnp.float32)[:, None] * frequency[None, :]
    cosines, sines = jnp.cos(angles), jnp.sin(angles)
    return (
        jnp.concatenate([cosines, cosines], axis=1),
        jnp.concatenate([-sines, sines], axis=1),
    )


def token_owners(page_table, lengths, pool_size, page_size):
    seq_count, max_pages = page_table.shape
    page_order = jnp.arange(max_pages, dtype=jnp.int32)
    used_pages = (lengths + page_size - 1) // page_size
    slot_ids = jnp.arange(pool_size, dtype=jnp.int32)
    matches = (page_table[:, :, None] == slot_ids[None, None, :]) & (
        page_order[None, :, None] < used_pages[:, None, None]
    )
    seq_ids = jnp.arange(seq_count, dtype=jnp.int32)
    owner = jnp.sum(jnp.where(matches, seq_ids[:, None, None], 0), axis=(0, 1))
    remaining = lengths[:, None] - page_order[None, :] * page_size
    visible = jnp.sum(jnp.where(matches, remaining[:, :, None], 0), axis=(0, 1))
    at = jnp.arange(page_size, dtype=jnp.int32)
    return jnp.where(at[None, :] < visible[:, None], owner[:, None], -1)


def attend_block(full_width, chunks, sums, table, owners, pages, out, *scratch):
    keys, values, scores, sems = scratch
    copies, seq_count, width = out.shape
    pool_size, page_size, head_size = keys.shape
    heads = width // head_size
    rows = heads * seq_count
    fetched = pool_size // sems.shape[1]
    slots = pool_size // chunks
    tokens = slots * page_size

    fetches = []
    for kind, held in enumerate((keys, values)):
        for k in range(pool_size // fetched):
            at = pl.ds(k * fetched, fetched)
            copy = pltpu.make_async_copy(pages.at[kind, 0, at], held.at[at], sems.at[kind, k])
            copy.start()
            fetches.append(copy)

    bias, cosines = table[:, :width], table[:, width : width + head_size]
    sines = table[:, width + head_size :]
    tail = sums[:, width:]
    lane = lax.broadcasted_iota(jnp.int32, tail.shape, 1)
    squares = jnp.sum(jnp.where(lane < 2, tail, 0.0), axis=1, keepdims=True)
    turned = sums[:, :width] * lax.rsqrt(squares / full_width + EPS) + bias
    pieces = []
    for k in range(heads):
        piece = turned[:, k * head_size : (k + 1) * head_size]
        across = pltpu.roll(piece, head_size // 2, 1)
        pieces.append(piece * cosines + across * sines)
    queries = jnp.concatenate(pieces, axis=0).astype(jnp.bfloat16)

    row_seq = lax.broadcasted_iota(jnp.int32, (rows, 1), 0) % seq_count
    highest = jnp.full((rows, head_size), -1e30, jnp.float32)
    for k in range(chunks):
        if k * slots % fetched == 0:
            fetches[k * slots // fetched].wait()
        key = keys[k * slots : (k + 1) * slots].reshape(tokens, head_size)
        here = lax.dot_general(
            queries, key, (((1,), (1,)), ((), ())), preferred_element_type=jnp.float32
        ) * (1.0 / math.sqrt(head_size))
        at = slice(k * tokens, (k + 1) * tokens)
        here = jnp.where(owners[:, at] == row_seq, here, -1e30)
        scores[:, at] = here
        for t in range(tokens // head_size):
            highest = jnp.maximum(highest, here[:, t * head_size : (t + 1) * head_size])
    highest = jnp.max(highest, axis=1, keepdims=True)
    summed = jnp.zeros((rows, head_size), jnp.float32)
    mixed = jnp.zeros((rows, head_size), jnp.float32)
    for k in range(chunks):
        powers = jnp.exp(scores[:, k * tokens : (k + 1) * tokens] - highest)
        for t in range(tokens // head_size):
            summed += powers[:, t * head_size : (t + 1) * head_size]
        if k * slots % fetched == 0:
            fetches[pool_size // fetched + k * slots // fetched].wait()
        value = values[k * slots : (k + 1) * slots].reshape(tokens, head_size)
        mixed += jnp.dot(powers.astype(jnp.bfloat16), value, preferred_element_type=jnp.float32)
    result = mixed / jnp.sum(summed, axis=1, keepdims=True)
    row = [result[k * seq_count : (k + 1) * seq_count] for k in range(heads)]
    row = jnp.concatenate(row, axis=1).astype(jnp.bfloat16)
    for k in range(copies):
        out[k] = row


def attend(sums, table, owners, page_cache, full_width, copies, fetches=1, chunks=4):
    seq_count, width = sums.shape
    width -= LANES
    pool_size, page_size, head_size = page_cache.shape[2:]
    pool = (pool_size, page_size, head_size)
    rows = width // head_size * seq_count
    in_hbm = pl.BlockSpec(memory_space=pltpu.HBM)
    in_vmem = pl.BlockSpec(memory_space=pltpu.VMEM)
    return pl.pallas_call(
        functools.partial(attend_block, full_width, chunks),
        in_specs=[in_vmem, in_vmem, in_vmem, in_hbm],
        out_specs=in_vmem,
        out_shape=pltpu.VMEM((copies, seq_count, width), jnp.bfloat16),
        scratch_shapes=[
            pltpu.VMEM(pool, jnp.bfloat16),
            pltpu.VMEM(pool, jnp.bfloat16),
            pltpu.VMEM((rows, pool_size * page_size), jnp.float32),
            pltpu.SemaphoreType.DMA((2, fetches)),
        ],
        compiler_params=pltpu.CompilerParams(vmem_limit_bytes=ATTEND_VMEM),
        interpret=INTERPRET,
        name="attend",
    )(near_by(sums), near_by(table), near_by(owners.reshape(1, -1)), far_off(page_cache))


def head_block(place, gathered, gain, near_weight, far_weight, *refs):
    batches, cores, per_batch, _, depth = gathered.shape
    side = (len(refs) - 2) // 2
    out_x, out_y = refs[:side], refs[side : 2 * side]
    weights, sems_in = refs[2 * side :]
    x_at, y_at, core_at = place[0], place[1], place[2]
    width = near_weight.shape[1] // (side * side * cores)
    rows_here = depth // cores

    def weight_copies(x_to, y_to):
        column = (((x_at + x_to) % side) * side + (y_at + y_to) % side) * cores + core_at
        column = pl.multiple_of(column * width, width)
        copies = []
        for k, (weight, core) in enumerate(((near_weight, core_at), (far_weight, 1 - core_at))):
            row = pl.multiple_of(core * rows_here, rows_here)
            copies.append(
                pltpu.make_async_copy(
                    weight.at[:, pl.ds(column, width)],
                    weights.at[x_to, pl.ds(row, rows_here), pl.ds(y_to * width, width)],
                    sems_in.at[x_to, y_to * 2 + k],
                )
            )
        return copies

    loads = [[c for y_to in range(side) for c in weight_copies(x_to, y_to)] for x_to in range(side)]
    for copies in loads:
        for copy in copies:
            copy.start()

    pieces = [
        gathered[b, c, i].astype(jnp.float32)
        for b in range(batches)
        for i in range(per_batch)
        for c in range(cores)
    ]
    ordered = jnp.concatenate(pieces, axis=0)
    features = ordered.astype(jnp.bfloat16)
    half = ordered.shape[0] // 2
    extra = out_x[0].shape[1] - half
    unscaled = ordered * (1.0 / gain[...])
    squares = jnp.sum(unscaled * unscaled, axis=1, keepdims=True)
    diagonal = lax.broadcasted_iota(jnp.int32, (half, half), 0) == lax.broadcasted_iota(
        jnp.int32, (half, half), 1
    )
    tails = []
    for part in (squares[:half], squares[half:]):
        line = jnp.sum(jnp.where(diagonal, part, 0.0), axis=0, keepdims=True)
        line = jnp.broadcast_to(line, (extra, half))
        coarse = line.astype(jnp.bfloat16)
        fine = (line - coarse.astype(jnp.float32)).astype(jnp.bfloat16)
        filler = jnp.zeros((extra, width - 2 * half), jnp.bfloat16)
        tails.append(jnp.concatenate([coarse, fine, filler], axis=1))
    tail_x, tail_y = tails

    for x_to in range(side):
        for copy in loads[x_to]:
            copy.wait()
        product = jnp.dot(features, weights[x_to], preferred_element_type=jnp.float32)
        for y_to in range(side):
            part = product[:, y_to * width : (y_to + 1) * width].astype(jnp.bfloat16)
            out_x[x_to][y_to, :half] = part[:half]
            out_x[x_to][y_to, half:] = tail_x
            out_y[y_to][x_to, :half] = part[half:]
            out_y[y_to][x_to, half:] = tail_y


def head_partials(gathered, gain, near_weight, far_weight, x_at, y_at, core_at, side):
    batches, cores, per_batch, seq_count, depth = gathered.shape
    half = batches * cores * per_batch * seq_count // 2
    width = near_weight.shape[1] // (side * side * cores)
    block = (side, half + 8, width)
    in_hbm = pl.BlockSpec(memory_space=pltpu.HBM)
    outs = pl.pallas_call(
        head_block,
        in_specs=[
            pl.BlockSpec(memory_space=pltpu.SMEM),
            pl.BlockSpec(memory_space=pltpu.VMEM),
            pl.BlockSpec(memory_space=pltpu.VMEM),
            in_hbm,
            in_hbm,
        ],
        out_shape=[pltpu.VMEM(block, jnp.bfloat16)] * (2 * side),
        scratch_shapes=[
            pltpu.VMEM((side, depth, side * width), jnp.bfloat16),
            pltpu.SemaphoreType.DMA((side, 2 * side)),
        ],
        compiler_params=pltpu.CompilerParams(vmem_limit_bytes=HEAD_VMEM),
        interpret=INTERPRET,
        name="head_partials",
    )(
        jnp.stack([x_at, y_at, core_at]).astype(jnp.int32),
        near_by(gathered),
        near_by(gain),
        far_off(near_weight),
        far_off(far_weight),
    )
    return outs[:side], outs[side:]


def summed_along(parts, axis):
    arrived = [shifted(parts[k], axis, k) for k in range(1, len(parts))]
    total = parts[0].astype(jnp.float32)
    for piece in arrived:
        total = total + piece.astype(jnp.float32)
    return total


def joined_all(top, total, axes):
    for axis in axes:
        pieces = sent_to_all(jnp.stack([top, total]), axis)
        tops = pieces[:, 0]
        top = jnp.max(tops, axis=0)
        total = jnp.sum(pieces[:, 1] * jnp.exp(tops - top[None]), axis=0)
    return top, total


def local(
    stream,
    input_gain,
    query_bias,
    query_weight,
    out_weight,
    page_cache,
    page_table,
    lengths,
    final_gain,
    head_weight,
):
    side, cores, batches = lax.axis_size("mp_0"), lax.axis_size("mp_2"), lax.axis_size("batch")
    members = side * side * cores
    x_at, y_at, core_at = lax.axis_index("mp_0"), lax.axis_index("mp_1"), lax.axis_index("mp_2")
    batch_at = lax.axis_index("batch")
    first_core = core_at == 0
    seqs, features_here = stream.shape
    full_width = features_here * members
    seq_count = page_table.shape[0]
    head_size = page_cache.shape[-1]

    far_head_weight = shifted(head_weight, "mp_2", 1)
    far_out_weight = shifted(out_weight, "mp_2", 1)

    parts = query_parts(stream, input_gain, query_weight).reshape(members, seq_count, -1)
    parts = lax.all_to_all(parts, MP, split_axis=0, concat_axis=0, tiled=True)
    owners = token_owners(page_table, lengths, *page_cache.shape[2:4])
    cosines, sines = turns(lengths - 1, head_size)
    bias = jnp.broadcast_to(query_bias[None], (seq_count, query_bias.shape[0]))
    table = jnp.concatenate([bias, cosines, sines], axis=1)
    sums = jnp.sum(parts.astype(jnp.float32), axis=0)
    attended = attend(
        sums, table, owners, page_cache, full_width, side * side
    )

    mine = lax.all_to_all(attended, XY, 0, 0, tiled=True).reshape(side * side * seq_count, -1)
    both_out = jnp.concatenate(
        [
            jnp.where(first_core, out_weight, far_out_weight),
            jnp.where(first_core, far_out_weight, out_weight),
        ],
        axis=1,
    )
    both_out = lax.optimization_barrier(both_out)
    partial_out = jnp.dot(mine, both_out, preferred_element_type=jnp.float32).astype(jnp.bfloat16)
    per_batch = side * side // batches
    arrived = lax.all_to_all(
        partial_out.reshape(batches, per_batch * seq_count, -1),
        "batch",
        split_axis=0,
        concat_axis=0,
        tiled=True,
    )
    rows = stream.reshape(batches, per_batch, cores, seq_count, features_here)
    rows = lax.dynamic_index_in_dim(rows, batch_at, 0, keepdims=False)

    def of_core(core):
        taken = lax.dynamic_index_in_dim(rows, core, 1, keepdims=False).reshape(-1, features_here)
        return jnp.concatenate([taken.astype(jnp.float32), final_gain[None]], axis=0)

    near_rows = of_core(core_at)
    far_rows = shifted(of_core(1 - core_at), "mp_2", 1)
    both = jnp.concatenate(
        [jnp.where(first_core, near_rows, far_rows), jnp.where(first_core, far_rows, near_rows)],
        axis=1,
    )
    residual = both[:-1] + jnp.sum(arrived.astype(jnp.float32), axis=0)
    payload = (residual * both[-1:]).astype(jnp.bfloat16)
    gathered = sent_to_all(payload, BATCH_CORE).reshape(batches, cores, per_batch, seq_count, -1)
    upper, lower = head_partials(
        gathered, both[-1:], head_weight, far_head_weight, x_at, y_at, core_at, side
    )
    upper = summed_along(upper, "mp_0").astype(jnp.bfloat16)
    lower = summed_along(lower, "mp_1").astype(jnp.bfloat16)
    upper = summed_along([upper[k] for k in range(side)], "mp_1")
    lower = summed_along([lower[k] for k in range(side)], "mp_0")

    def rescaled(total):
        half = seqs // 2
        squares = total[half, :half] + total[half, half : 2 * half]
        return total[:half] * lax.rsqrt(squares / full_width + EPS)[:, None]

    logits = jnp.concatenate([rescaled(upper), rescaled(lower)], axis=0)

    local_top = jnp.max(logits, axis=1)
    local_sum = jnp.sum(jnp.exp(logits - local_top[:, None]), axis=1)
    highest, summed = joined_all(local_top, local_sum, (MP, "batch"))
    return (logits, jnp.log(summed) + highest)


def solution(mesh):
    torus = Mesh(
        mesh.devices.reshape(mesh.shape["batch"], 4, 4, 2), ("batch", "mp_0", "mp_1", "mp_2")
    )
    in_specs = (
        P(None, MP),
        P(MP),
        P("batch"),
        P(MP, "batch"),
        P("batch", MP),
        P(None, "batch", MP, None, None),
        P(MP, None),
        P(MP),
        P(MP),
        P(MP, "batch"),
    )
    out_specs = (P(None, BATCH_MP), P())

    def step(*args):
        return local(*args)

    step = jax.shard_map(step, mesh=torus, in_specs=in_specs, out_specs=out_specs, check_vma=False)
    return step
```

```python
import functools
import math

import jax
import jax.numpy as jnp
from jax import lax
from jax.experimental import pallas as pl
from jax.experimental.pallas import tpu as pltpu
from jax.sharding import Mesh
from jax.sharding import PartitionSpec as P

MP = ("mp_0", "mp_1", "mp_2")
BATCH_MP = ("batch", "mp_0", "mp_1", "mp_2")
XY = ("mp_0", "mp_1")
BATCH_CORE = ("batch", "mp_2")


EPS = 1e-06
ROPE_BASE = 1000000.0
INTERPRET = False

LANES = 128
HEAD_VMEM = 24 * 2**20
ATTEND_VMEM = 16 * 2**20


def near_by(x):
    return pltpu.with_memory_space_constraint(x, pltpu.VMEM)


def far_off(x):
    return pltpu.with_memory_space_constraint(x, pltpu.HBM)


def sent_to_all(x, axis):
    length = lax.axis_size(axis)
    return lax.all_to_all(jnp.broadcast_to(x[None], (length, *x.shape)), axis, 0, 0, tiled=True)


def shifted(x, axis, by):
    length = lax.axis_size(axis)
    return lax.ppermute(x, axis, [(k, (k + by) % length) for k in range(length)])


def query_block(stream, gain, weight, out):
    width = weight.shape[1]
    features = stream[...].astype(jnp.float32)
    squares = jnp.sum(features * features, axis=1, keepdims=True)
    products = jnp.dot(
        (features * gain[...]).astype(jnp.bfloat16), weight[...], preferred_element_type=jnp.float32
    )
    out[:, :width] = products.astype(jnp.bfloat16)
    coarse = squares.astype(jnp.bfloat16).astype(jnp.float32)
    lane = lax.broadcasted_iota(jnp.int32, (features.shape[0], LANES), 1)
    tail = jnp.where(lane == 0, coarse, jnp.where(lane == 1, squares - coarse, 0.0))
    out[:, width:] = tail.astype(jnp.bfloat16)


def query_parts(stream, gain, weight):
    return pl.pallas_call(
        query_block,
        out_shape=pltpu.VMEM((stream.shape[0], weight.shape[1] + LANES), jnp.bfloat16),
        interpret=INTERPRET,
        name="query_parts",
    )(stream, gain[None], weight)


def turns(position, head_size):
    half_dim = head_size // 2
    exponent = jnp.arange(half_dim, dtype=jnp.float32) * (-2.0 / head_size)
    frequency = ROPE_BASE**exponent
    angles = position.astype(jnp.float32)[:, None] * frequency[None, :]
    cosines, sines = jnp.cos(angles), jnp.sin(angles)
    return (
        jnp.concatenate([cosines, cosines], axis=1),
        jnp.concatenate([-sines, sines], axis=1),
    )


def token_owners(page_table, lengths, pool_size, page_size):
    seq_count, max_pages = page_table.shape
    page_order = jnp.arange(max_pages, dtype=jnp.int32)
    used_pages = (lengths + page_size - 1) // page_size
    slot_ids = jnp.arange(pool_size, dtype=jnp.int32)
    matches = (page_table[:, :, None] == slot_ids[None, None, :]) & (
        page_order[None, :, None] < used_pages[:, None, None]
    )
    seq_ids = jnp.arange(seq_count, dtype=jnp.int32)
    owner = jnp.sum(jnp.where(matches, seq_ids[:, None, None], 0), axis=(0, 1))
    remaining = lengths[:, None] - page_order[None, :] * page_size
    visible = jnp.sum(jnp.where(matches, remaining[:, :, None], 0), axis=(0, 1))
    at = jnp.arange(page_size, dtype=jnp.int32)
    return jnp.where(at[None, :] < visible[:, None], owner[:, None], -1)


def attend_block(full_width, chunks, sums, table, owners, pages, out, *scratch):
    keys, values, scores, sems = scratch
    copies, seq_count, width = out.shape
    pool_size, page_size, head_size = keys.shape
    heads = width // head_size
    rows = heads * seq_count
    fetched = pool_size // sems.shape[1]
    slots = pool_size // chunks
    tokens = slots * page_size

    fetches = []
    for kind, held in enumerate((keys, values)):
        for k in range(pool_size // fetched):
            at = pl.ds(k * fetched, fetched)
            copy = pltpu.make_async_copy(pages.at[kind, 0, at], held.at[at], sems.at[kind, k])
            copy.start()
            fetches.append(copy)

    bias, cosines = table[:, :width], table[:, width : width + head_size]
    sines = table[:, width + head_size :]
    tail = sums[:, width:]
    lane = lax.broadcasted_iota(jnp.int32, tail.shape, 1)
    squares = jnp.sum(jnp.where(lane < 2, tail, 0.0), axis=1, keepdims=True)
    turned = sums[:, :width] * lax.rsqrt(squares / full_width + EPS) + bias
    pieces = []
    for k in range(heads):
        piece = turned[:, k * head_size : (k + 1) * head_size]
        across = pltpu.roll(piece, head_size // 2, 1)
        pieces.append(piece * cosines + across * sines)
    queries = jnp.concatenate(pieces, axis=0).astype(jnp.bfloat16)

    row_seq = lax.broadcasted_iota(jnp.int32, (rows, 1), 0) % seq_count
    highest = jnp.full((rows, head_size), -1e30, jnp.float32)
    for k in range(chunks):
        if k * slots % fetched == 0:
            fetches[k * slots // fetched].wait()
        key = keys[k * slots : (k + 1) * slots].reshape(tokens, head_size)
        here = lax.dot_general(
            queries, key, (((1,), (1,)), ((), ())), preferred_element_type=jnp.float32
        ) * (1.0 / math.sqrt(head_size))
        at = slice(k * tokens, (k + 1) * tokens)
        here = jnp.where(owners[:, at] == row_seq, here, -1e30)
        scores[:, at] = here
        for t in range(tokens // head_size):
            highest = jnp.maximum(highest, here[:, t * head_size : (t + 1) * head_size])
    highest = jnp.max(highest, axis=1, keepdims=True)
    summed = jnp.zeros((rows, head_size), jnp.float32)
    mixed = jnp.zeros((rows, head_size), jnp.float32)
    for k in range(chunks):
        powers = jnp.exp(scores[:, k * tokens : (k + 1) * tokens] - highest)
        for t in range(tokens // head_size):
            summed += powers[:, t * head_size : (t + 1) * head_size]
        if k * slots % fetched == 0:
            fetches[pool_size // fetched + k * slots // fetched].wait()
        value = values[k * slots : (k + 1) * slots].reshape(tokens, head_size)
        mixed += jnp.dot(powers.astype(jnp.bfloat16), value, preferred_element_type=jnp.float32)
    result = mixed / jnp.sum(summed, axis=1, keepdims=True)
    row = [result[k * seq_count : (k + 1) * seq_count] for k in range(heads)]
    row = jnp.concatenate(row, axis=1).astype(jnp.bfloat16)
    for k in range(copies):
        out[k] = row


def attend(sums, table, owners, page_cache, full_width, copies, fetches=1, chunks=4):
    seq_count, width = sums.shape
    width -= LANES
    pool_size, page_size, head_size = page_cache.shape[2:]
    pool = (pool_size, page_size, head_size)
    rows = width // head_size * seq_count
    in_hbm = pl.BlockSpec(memory_space=pltpu.HBM)
    in_vmem = pl.BlockSpec(memory_space=pltpu.VMEM)
    return pl.pallas_call(
        functools.partial(attend_block, full_width, chunks),
        in_specs=[in_vmem, in_vmem, in_vmem, in_hbm],
        out_specs=in_vmem,
        out_shape=pltpu.VMEM((copies, seq_count, width), jnp.bfloat16),
        scratch_shapes=[
            pltpu.VMEM(pool, jnp.bfloat16),
            pltpu.VMEM(pool, jnp.bfloat16),
            pltpu.VMEM((rows, pool_size * page_size), jnp.float32),
            pltpu.SemaphoreType.DMA((2, fetches)),
        ],
        compiler_params=pltpu.CompilerParams(vmem_limit_bytes=ATTEND_VMEM),
        interpret=INTERPRET,
        name="attend",
    )(near_by(sums), near_by(table), near_by(owners.reshape(1, -1)), far_off(page_cache))


def in_order(gathered):
    batches, cores, per_batch, _, _ = gathered.shape
    pieces = [
        gathered[b, c, i].astype(jnp.float32)
        for b in range(batches)
        for i in range(per_batch)
        for c in range(cores)
    ]
    return jnp.concatenate(pieces, axis=0)


def squares_line(rows, gain):
    unscaled = rows * (1.0 / gain)
    squares = jnp.sum(unscaled * unscaled, axis=1, keepdims=True)
    shape = (rows.shape[0], rows.shape[0])
    diagonal = lax.broadcasted_iota(jnp.int32, shape, 0) == lax.broadcasted_iota(jnp.int32, shape, 1)
    return jnp.sum(jnp.where(diagonal, squares, 0.0), axis=0, keepdims=True)


def head_block(place, gathered, gain, near_weight, far_weight, *refs):
    _, cores, _, _, depth = gathered.shape
    side = len(refs) // 2
    out_x, out_y = refs[: side - 1], refs[side - 1 : 2 * side - 2]
    weights, sems_in = refs[2 * side - 2 :]
    held = [k for k in range(side) if k != side // 2]
    x_at, y_at, core_at = place[0], place[1], place[2]
    width = near_weight.shape[1] // (side * side * cores)
    rows_here = depth // cores

    def weight_copies(x_to, y_to):
        column = (((x_at + x_to) % side) * side + (y_at + y_to) % side) * cores + core_at
        column = pl.multiple_of(column * width, width)
        copies = []
        for k, (weight, core) in enumerate(((near_weight, core_at), (far_weight, 1 - core_at))):
            row = pl.multiple_of(core * rows_here, rows_here)
            copies.append(
                pltpu.make_async_copy(
                    weight.at[:, pl.ds(column, width)],
                    weights.at[x_to, pl.ds(row, rows_here), pl.ds(y_to * width, width)],
                    sems_in.at[x_to, y_to * 2 + k],
                )
            )
        return copies

    loads = [[c for y_to in range(side) for c in weight_copies(x_to, y_to)] for x_to in range(side)]
    for copies in loads:
        for copy in copies:
            copy.start()

    ordered = in_order(gathered)
    features = ordered.astype(jnp.bfloat16)
    half = ordered.shape[0] // 2
    extra = out_x[0].shape[1] - half
    tails = []
    for part in (ordered[:half], ordered[half:]):
        line = jnp.broadcast_to(squares_line(part, gain[...]), (extra, half))
        coarse = line.astype(jnp.bfloat16)
        fine = (line - coarse.astype(jnp.float32)).astype(jnp.bfloat16)
        filler = jnp.zeros((extra, width - 2 * half), jnp.bfloat16)
        tails.append(jnp.concatenate([coarse, fine, filler], axis=1))
    tail_x, tail_y = tails

    for x_to in range(side):
        for copy in loads[x_to]:
            copy.wait()
        product = jnp.dot(features, weights[x_to], preferred_element_type=jnp.float32)
        for y_to in range(side):
            part = product[:, y_to * width : (y_to + 1) * width].astype(jnp.bfloat16)
            if x_to in held:
                out_x[held.index(x_to)][y_to, :half] = part[:half]
                out_x[held.index(x_to)][y_to, half:] = tail_x
            if y_to in held:
                out_y[held.index(y_to)][x_to, :half] = part[half:]
                out_y[held.index(y_to)][x_to, half:] = tail_y


def head_partials(gathered, gain, near_weight, far_weight, place, side):
    batches, cores, per_batch, seq_count, depth = gathered.shape
    half = batches * cores * per_batch * seq_count // 2
    width = near_weight.shape[1] // (side * side * cores)
    block = (side, half + 8, width)
    in_hbm = pl.BlockSpec(memory_space=pltpu.HBM)
    outs = pl.pallas_call(
        head_block,
        in_specs=[
            pl.BlockSpec(memory_space=pltpu.SMEM),
            pl.BlockSpec(memory_space=pltpu.VMEM),
            pl.BlockSpec(memory_space=pltpu.VMEM),
            in_hbm,
            in_hbm,
        ],
        out_shape=[pltpu.VMEM(block, jnp.bfloat16)] * (2 * side - 2),
        scratch_shapes=[
            pltpu.VMEM((side, depth, side * width), jnp.bfloat16),
            pltpu.SemaphoreType.DMA((side, 2 * side)),
        ],
        compiler_params=pltpu.CompilerParams(vmem_limit_bytes=HEAD_VMEM),
        interpret=INTERPRET,
        name="head_partials",
    )(
        place,
        near_by(gathered),
        near_by(gain),
        far_off(near_weight),
        far_off(far_weight),
    )
    return outs[: side - 1], outs[side - 1 :]


def partner_weights_block(sizes, place, near_weight, far_weight, out_x, out_y, held, sems, sems_out):
    side, cores, width = sizes
    rows_here = near_weight.shape[0]
    x_at, y_at, core_at = place[0], place[1], place[2]
    copies = []
    for t in range(side):
        places = (
            ((x_at + side // 2) % side, (y_at + t) % side),
            ((x_at + t) % side, (y_at + side // 2) % side),
        )
        for way, (x_to, y_to) in enumerate(places):
            column = pl.multiple_of(((x_to * side + y_to) * cores + core_at) * width, width)
            for k, weight in enumerate((near_weight, far_weight)):
                copy = pltpu.make_async_copy(
                    weight.at[:, pl.ds(column, width)],
                    held.at[way, pl.ds(k * rows_here, rows_here), pl.ds(t * width, width)],
                    sems.at[way, k, t],
                )
                copy.start()
                copies.append(copy)
    for copy in copies:
        copy.wait()
    stores = [
        pltpu.make_async_copy(held.at[way], out, sems_out.at[way])
        for way, out in enumerate((out_x, out_y))
    ]
    for copy in stores:
        copy.start()
    for copy in stores:
        copy.wait()


def partner_weights(near_weight, far_weight, place, side, cores):
    rows_here, columns = near_weight.shape
    width = columns // (side * side * cores)
    shape = (cores * rows_here, side * width)
    in_hbm = pl.BlockSpec(memory_space=pltpu.HBM)
    return pl.pallas_call(
        functools.partial(partner_weights_block, (side, cores, width)),
        in_specs=[pl.BlockSpec(memory_space=pltpu.SMEM), in_hbm, in_hbm],
        out_specs=[in_hbm, in_hbm],
        out_shape=[pltpu.HBM(shape, jnp.bfloat16)] * 2,
        scratch_shapes=[
            pltpu.VMEM((2, *shape), jnp.bfloat16),
            pltpu.SemaphoreType.DMA((2, cores, side)),
            pltpu.SemaphoreType.DMA((2,)),
        ],
        compiler_params=pltpu.CompilerParams(vmem_limit_bytes=ATTEND_VMEM),
        interpret=INTERPRET,
        name="partner_weights",
    )(place, far_off(near_weight), far_off(far_weight))


def head_partner_block(core, rows_x, rows_y, gain_x, gain_y, weight_x, weight_y, *outs):
    weights = (weight_x, weight_y)
    rows_here = rows_x.shape[-1] // 2
    first_core = core[0] == 0
    for way, (rows, gain) in enumerate(((rows_x, gain_x), (rows_y, gain_y))):
        side, tall, width = outs[way].shape
        ordered = in_order(rows)
        half = ordered.shape[0]
        line = jnp.broadcast_to(squares_line(ordered, gain[...]), (tall - half, half))
        tail = jnp.concatenate(
            [line, jnp.zeros((tall - half, width - half), jnp.float32)], axis=1
        )
        sides = (ordered[:, :rows_here], ordered[:, rows_here:])
        near = jnp.where(first_core, sides[0], sides[1])
        far = jnp.where(first_core, sides[1], sides[0])
        features = jnp.concatenate([near, far], axis=1).astype(jnp.bfloat16)
        product = jnp.dot(features, weights[way][...], preferred_element_type=jnp.float32)
        for t in range(side):
            outs[way][t, :half] = product[:, t * width : (t + 1) * width]
            outs[way][t, half:] = tail


def head_partner(rows_x, rows_y, gain_x, gain_y, weight_x, weight_y, core_at, side):
    depth, columns = weight_x.shape
    half = rows_x.size // depth
    block = (side, half + 8, columns // side)
    in_vmem = pl.BlockSpec(memory_space=pltpu.VMEM)
    return pl.pallas_call(
        head_partner_block,
        in_specs=[pl.BlockSpec(memory_space=pltpu.SMEM), *[in_vmem] * 6],
        out_shape=[pltpu.VMEM(block, jnp.float32)] * 2,
        compiler_params=pltpu.CompilerParams(vmem_limit_bytes=ATTEND_VMEM),
        interpret=INTERPRET,
        name="head_partner",
    )(
        core_at.astype(jnp.int32)[None],
        *(near_by(x) for x in (rows_x, rows_y, gain_x, gain_y, weight_x, weight_y)),
    )


def summed_along(parts, axis):
    arrived = [shifted(parts[k], axis, k) for k in range(1, len(parts))]
    total = parts[0].astype(jnp.float32)
    for piece in arrived:
        total = total + piece.astype(jnp.float32)
    return total


def summed_near(parts, partner, axis):
    side = lax.axis_size(axis)
    arrived = [shifted(parts[-1 if k > 1 else 1], axis, k) for k in (1, side - 1)]
    total = parts[0].astype(jnp.float32) + partner
    for piece in arrived:
        total = total + piece.astype(jnp.float32)
    return total


def joined_all(top, total, axes):
    for axis in axes:
        pieces = sent_to_all(jnp.stack([top, total]), axis)
        tops = pieces[:, 0]
        top = jnp.max(tops, axis=0)
        total = jnp.sum(pieces[:, 1] * jnp.exp(tops - top[None]), axis=0)
    return top, total


def local(
    stream,
    input_gain,
    query_bias,
    query_weight,
    out_weight,
    page_cache,
    page_table,
    lengths,
    final_gain,
    head_weight,
):
    side, cores, batches = lax.axis_size("mp_0"), lax.axis_size("mp_2"), lax.axis_size("batch")
    members = side * side * cores
    x_at, y_at, core_at = lax.axis_index("mp_0"), lax.axis_index("mp_1"), lax.axis_index("mp_2")
    batch_at = lax.axis_index("batch")
    first_core = core_at == 0
    seqs, features_here = stream.shape
    full_width = features_here * members
    seq_count = page_table.shape[0]
    head_size = page_cache.shape[-1]

    far_head_weight = shifted(head_weight, "mp_2", 1)
    far_out_weight = shifted(out_weight, "mp_2", 1)

    parts = query_parts(stream, input_gain, query_weight).reshape(members, seq_count, -1)
    parts = lax.all_to_all(parts, MP, split_axis=0, concat_axis=0, tiled=True)
    owners = token_owners(page_table, lengths, *page_cache.shape[2:4])
    cosines, sines = turns(lengths - 1, head_size)
    bias = jnp.broadcast_to(query_bias[None], (seq_count, query_bias.shape[0]))
    table = jnp.concatenate([bias, cosines, sines], axis=1)
    sums = jnp.sum(parts.astype(jnp.float32), axis=0)
    attended = attend(
        sums, table, owners, page_cache, full_width, side * side
    )

    mine = lax.all_to_all(attended, XY, 0, 0, tiled=True)
    place = jnp.stack([x_at, y_at, core_at]).astype(jnp.int32)
    weight_x, weight_y = partner_weights(head_weight, far_head_weight, place, side, cores)
    weight_x = shifted(weight_x, "mp_0", side // 2)
    weight_y = shifted(weight_y, "mp_1", side // 2)
    mine = mine.reshape(side * side * seq_count, -1)
    near_out = jnp.dot(mine, out_weight, preferred_element_type=jnp.float32)
    far_out = jnp.dot(mine, far_out_weight, preferred_element_type=jnp.float32)
    partial_out = jnp.concatenate(
        [jnp.where(first_core, near_out, far_out), jnp.where(first_core, far_out, near_out)], axis=1
    ).astype(jnp.bfloat16)
    per_batch = side * side // batches
    arrived = lax.all_to_all(
        partial_out.reshape(batches, per_batch * seq_count, -1),
        "batch",
        split_axis=0,
        concat_axis=0,
        tiled=True,
    )
    rows = stream.reshape(batches, per_batch, cores, seq_count, features_here)
    rows = lax.dynamic_index_in_dim(rows, batch_at, 0, keepdims=False)

    def of_core(core):
        taken = lax.dynamic_index_in_dim(rows, core, 1, keepdims=False).reshape(-1, features_here)
        return jnp.concatenate([taken.astype(jnp.float32), final_gain[None]], axis=0)

    near_rows = of_core(core_at)
    far_rows = shifted(of_core(1 - core_at), "mp_2", 1)
    both = jnp.concatenate(
        [jnp.where(first_core, near_rows, far_rows), jnp.where(first_core, far_rows, near_rows)],
        axis=1,
    )
    residual = both[:-1] + jnp.sum(arrived.astype(jnp.float32), axis=0)
    payload = (residual * both[-1:]).astype(jnp.bfloat16)
    gathered = sent_to_all(payload, BATCH_CORE)
    gathered = gathered.reshape(batches, cores, per_batch, seq_count, -1)
    rows_x = shifted(gathered[: batches // 2], "mp_0", side // 2)
    rows_y = shifted(gathered[batches // 2 :], "mp_1", side // 2)
    gain = both[-1:]
    gain_x = shifted(gain, "mp_0", side // 2)
    gain_y = shifted(gain, "mp_1", side // 2)
    upper, lower = head_partials(gathered, gain, head_weight, far_head_weight, place, side)
    partner_x, partner_y = head_partner(
        rows_x, rows_y, gain_x, gain_y, weight_x, weight_y, core_at, side
    )
    upper = summed_near(upper, partner_x, "mp_0").astype(jnp.bfloat16)
    lower = summed_near(lower, partner_y, "mp_1").astype(jnp.bfloat16)
    upper = summed_along([upper[k] for k in range(side)], "mp_1")
    lower = summed_along([lower[k] for k in range(side)], "mp_0")

    def rescaled(total):
        half = seqs // 2
        squares = total[half, :half] + total[half, half : 2 * half]
        return total[:half] * lax.rsqrt(squares / full_width + EPS)[:, None]

    logits = jnp.concatenate([rescaled(upper), rescaled(lower)], axis=0)

    local_top = jnp.max(logits, axis=1)
    local_sum = jnp.sum(jnp.exp(logits - local_top[:, None]), axis=1)
    highest, summed = joined_all(local_top, local_sum, (MP, "batch"))
    return (logits, jnp.log(summed) + highest)


def solution(mesh):
    torus = Mesh(
        mesh.devices.reshape(mesh.shape["batch"], 4, 4, 2), ("batch", "mp_0", "mp_1", "mp_2")
    )
    in_specs = (
        P(None, MP),
        P(MP),
        P("batch"),
        P(MP, "batch"),
        P("batch", MP),
        P(None, "batch", MP, None, None),
        P(MP, None),
        P(MP),
        P(MP),
        P(MP, "batch"),
    )
    out_specs = (P(None, BATCH_MP), P())

    def step(*args):
        return local(*args)

    step = jax.shard_map(step, mesh=torus, in_specs=in_specs, out_specs=out_specs, check_vma=False)
    return step
```

```python
import functools
import math

import jax
import jax.numpy as jnp
from jax import lax
from jax.experimental import pallas as pl
from jax.experimental.pallas import tpu as pltpu
from jax.sharding import Mesh
from jax.sharding import PartitionSpec as P

MP = ("mp_0", "mp_1", "mp_2")
BATCH_MP = ("batch", "mp_0", "mp_1", "mp_2")
XY = ("mp_0", "mp_1")
BATCH_CORE = ("batch", "mp_2")


EPS = 1e-06
ROPE_BASE = 1000000.0
INTERPRET = False

LANES = 128
HEAD_VMEM = 24 * 2**20
ATTEND_VMEM = 16 * 2**20


def near_by(x):
    return pltpu.with_memory_space_constraint(x, pltpu.VMEM)


def far_off(x):
    return pltpu.with_memory_space_constraint(x, pltpu.HBM)


def sent_to_all(x, axis):
    length = lax.axis_size(axis)
    return lax.all_to_all(jnp.broadcast_to(x[None], (length, *x.shape)), axis, 0, 0, tiled=True)


def shifted(x, axis, by):
    length = lax.axis_size(axis)
    return lax.ppermute(x, axis, [(k, (k + by) % length) for k in range(length)])


def query_block(stream, gain, weight, out):
    width = weight.shape[1]
    features = stream[...].astype(jnp.float32)
    squares = jnp.sum(features * features, axis=1, keepdims=True)
    products = jnp.dot(
        (features * gain[...]).astype(jnp.bfloat16), weight[...], preferred_element_type=jnp.float32
    )
    out[:, :width] = products.astype(jnp.bfloat16)
    coarse = squares.astype(jnp.bfloat16).astype(jnp.float32)
    lane = lax.broadcasted_iota(jnp.int32, (features.shape[0], LANES), 1)
    tail = jnp.where(lane == 0, coarse, jnp.where(lane == 1, squares - coarse, 0.0))
    out[:, width:] = tail.astype(jnp.bfloat16)


def query_parts(stream, gain, weight):
    return pl.pallas_call(
        query_block,
        out_shape=pltpu.VMEM((stream.shape[0], weight.shape[1] + LANES), jnp.bfloat16),
        interpret=INTERPRET,
        name="query_parts",
    )(stream, gain[None], weight)


def turns(position, head_size):
    half_dim = head_size // 2
    exponent = jnp.arange(half_dim, dtype=jnp.float32) * (-2.0 / head_size)
    frequency = ROPE_BASE**exponent
    angles = position.astype(jnp.float32)[:, None] * frequency[None, :]
    cosines, sines = jnp.cos(angles), jnp.sin(angles)
    return (
        jnp.concatenate([cosines, cosines], axis=1),
        jnp.concatenate([-sines, sines], axis=1),
    )


def token_owners(page_table, lengths, pool_size, page_size):
    seq_count, max_pages = page_table.shape
    page_order = jnp.arange(max_pages, dtype=jnp.int32)
    used_pages = (lengths + page_size - 1) // page_size
    slot_ids = jnp.arange(pool_size, dtype=jnp.int32)
    matches = (page_table[:, :, None] == slot_ids[None, None, :]) & (
        page_order[None, :, None] < used_pages[:, None, None]
    )
    seq_ids = jnp.arange(seq_count, dtype=jnp.int32)
    owner = jnp.sum(jnp.where(matches, seq_ids[:, None, None], 0), axis=(0, 1))
    remaining = lengths[:, None] - page_order[None, :] * page_size
    visible = jnp.sum(jnp.where(matches, remaining[:, :, None], 0), axis=(0, 1))
    at = jnp.arange(page_size, dtype=jnp.int32)
    return jnp.where(at[None, :] < visible[:, None], owner[:, None], -1)


def attend_block(full_width, chunks, sums, table, owners, pages, out, *scratch):
    keys, values, scores, sems = scratch
    copies, seq_count, width = out.shape
    pool_size, page_size, head_size = keys.shape
    heads = width // head_size
    rows = heads * seq_count
    fetched = pool_size // sems.shape[1]
    slots = pool_size // chunks
    tokens = slots * page_size

    fetches = []
    for kind, held in enumerate((keys, values)):
        for k in range(pool_size // fetched):
            at = pl.ds(k * fetched, fetched)
            copy = pltpu.make_async_copy(pages.at[kind, 0, at], held.at[at], sems.at[kind, k])
            copy.start()
            fetches.append(copy)

    bias, cosines = table[:, :width], table[:, width : width + head_size]
    sines = table[:, width + head_size :]
    tail = sums[:, width:]
    lane = lax.broadcasted_iota(jnp.int32, tail.shape, 1)
    squares = jnp.sum(jnp.where(lane < 2, tail, 0.0), axis=1, keepdims=True)
    turned = sums[:, :width] * lax.rsqrt(squares / full_width + EPS) + bias
    pieces = []
    for k in range(heads):
        piece = turned[:, k * head_size : (k + 1) * head_size]
        across = pltpu.roll(piece, head_size // 2, 1)
        pieces.append(piece * cosines + across * sines)
    queries = jnp.concatenate(pieces, axis=0).astype(jnp.bfloat16)

    row_seq = lax.broadcasted_iota(jnp.int32, (rows, 1), 0) % seq_count
    highest = jnp.full((rows, head_size), -1e30, jnp.float32)
    for k in range(chunks):
        if k * slots % fetched == 0:
            fetches[k * slots // fetched].wait()
        key = keys[k * slots : (k + 1) * slots].reshape(tokens, head_size)
        here = lax.dot_general(
            queries, key, (((1,), (1,)), ((), ())), preferred_element_type=jnp.float32
        ) * (1.0 / math.sqrt(head_size))
        at = slice(k * tokens, (k + 1) * tokens)
        here = jnp.where(owners[:, at] == row_seq, here, -1e30)
        scores[:, at] = here
        for t in range(tokens // head_size):
            highest = jnp.maximum(highest, here[:, t * head_size : (t + 1) * head_size])
    highest = jnp.max(highest, axis=1, keepdims=True)
    summed = jnp.zeros((rows, head_size), jnp.float32)
    mixed = jnp.zeros((rows, head_size), jnp.float32)
    for k in range(chunks):
        powers = jnp.exp(scores[:, k * tokens : (k + 1) * tokens] - highest)
        for t in range(tokens // head_size):
            summed += powers[:, t * head_size : (t + 1) * head_size]
        if k * slots % fetched == 0:
            fetches[pool_size // fetched + k * slots // fetched].wait()
        value = values[k * slots : (k + 1) * slots].reshape(tokens, head_size)
        mixed += jnp.dot(powers.astype(jnp.bfloat16), value, preferred_element_type=jnp.float32)
    result = mixed / jnp.sum(summed, axis=1, keepdims=True)
    row = [result[k * seq_count : (k + 1) * seq_count] for k in range(heads)]
    row = jnp.concatenate(row, axis=1).astype(jnp.bfloat16)
    for k in range(copies):
        out[k] = row


def attend(sums, table, owners, page_cache, full_width, copies, fetches=1, chunks=4):
    seq_count, width = sums.shape
    width -= LANES
    pool_size, page_size, head_size = page_cache.shape[2:]
    pool = (pool_size, page_size, head_size)
    rows = width // head_size * seq_count
    in_hbm = pl.BlockSpec(memory_space=pltpu.HBM)
    in_vmem = pl.BlockSpec(memory_space=pltpu.VMEM)
    return pl.pallas_call(
        functools.partial(attend_block, full_width, chunks),
        in_specs=[in_vmem, in_vmem, in_vmem, in_hbm],
        out_specs=in_vmem,
        out_shape=pltpu.VMEM((copies, seq_count, width), jnp.bfloat16),
        scratch_shapes=[
            pltpu.VMEM(pool, jnp.bfloat16),
            pltpu.VMEM(pool, jnp.bfloat16),
            pltpu.VMEM((rows, pool_size * page_size), jnp.float32),
            pltpu.SemaphoreType.DMA((2, fetches)),
        ],
        compiler_params=pltpu.CompilerParams(vmem_limit_bytes=ATTEND_VMEM),
        interpret=INTERPRET,
        name="attend",
    )(near_by(sums), near_by(table), near_by(owners.reshape(1, -1)), far_off(page_cache))


def in_order(gathered):
    batches, cores, per_batch, _, _ = gathered.shape
    pieces = [
        gathered[b, c, i].astype(jnp.float32)
        for b in range(batches)
        for i in range(per_batch)
        for c in range(cores)
    ]
    return jnp.concatenate(pieces, axis=0)


def squares_line(rows, gain):
    unscaled = rows * (1.0 / gain)
    squares = jnp.sum(unscaled * unscaled, axis=1, keepdims=True)
    shape = (rows.shape[0], rows.shape[0])
    diagonal = lax.broadcasted_iota(jnp.int32, shape, 0) == lax.broadcasted_iota(jnp.int32, shape, 1)
    return jnp.sum(jnp.where(diagonal, squares, 0.0), axis=0, keepdims=True)


def head_block(place, gathered, gain, near_weight, far_weight, *refs):
    _, cores, _, _, depth = gathered.shape
    side = len(refs) // 2
    out_x, out_y = refs[: side - 1], refs[side - 1 : 2 * side - 2]
    weights, sems_in = refs[2 * side - 2 :]
    held = [k for k in range(side) if k != side // 2]
    x_at, y_at, core_at = place[0], place[1], place[2]
    width = near_weight.shape[1] // (side * side * cores)
    rows_here = depth // cores

    def weight_copies(x_to, y_to):
        column = (((x_at + x_to) % side) * side + (y_at + y_to) % side) * cores + core_at
        column = pl.multiple_of(column * width, width)
        copies = []
        for k, (weight, core) in enumerate(((near_weight, core_at), (far_weight, 1 - core_at))):
            row = pl.multiple_of(core * rows_here, rows_here)
            copies.append(
                pltpu.make_async_copy(
                    weight.at[:, pl.ds(column, width)],
                    weights.at[x_to, pl.ds(row, rows_here), pl.ds(y_to * width, width)],
                    sems_in.at[x_to, y_to * 2 + k],
                )
            )
        return copies

    loads = [[c for y_to in range(side) for c in weight_copies(x_to, y_to)] for x_to in range(side)]
    for copies in loads:
        for copy in copies:
            copy.start()

    ordered = in_order(gathered)
    features = ordered.astype(jnp.bfloat16)
    half = ordered.shape[0] // 2
    extra = out_x[0].shape[1] - half
    tails = []
    for part in (ordered[:half], ordered[half:]):
        line = jnp.broadcast_to(squares_line(part, gain[...]), (extra, half))
        coarse = line.astype(jnp.bfloat16)
        fine = (line - coarse.astype(jnp.float32)).astype(jnp.bfloat16)
        filler = jnp.zeros((extra, width - 2 * half), jnp.bfloat16)
        tails.append(jnp.concatenate([coarse, fine, filler], axis=1))
    tail_x, tail_y = tails

    for x_to in range(side):
        for copy in loads[x_to]:
            copy.wait()
        product = jnp.dot(features, weights[x_to], preferred_element_type=jnp.float32)
        for y_to in range(side):
            part = product[:, y_to * width : (y_to + 1) * width].astype(jnp.bfloat16)
            if x_to in held:
                out_x[held.index(x_to)][y_to, :half] = part[:half]
                out_x[held.index(x_to)][y_to, half:] = tail_x
            if y_to in held:
                out_y[held.index(y_to)][x_to, :half] = part[half:]
                out_y[held.index(y_to)][x_to, half:] = tail_y


def head_partials(gathered, gain, near_weight, far_weight, place, side):
    batches, cores, per_batch, seq_count, depth = gathered.shape
    half = batches * cores * per_batch * seq_count // 2
    width = near_weight.shape[1] // (side * side * cores)
    block = (side, half + 8, width)
    in_hbm = pl.BlockSpec(memory_space=pltpu.HBM)
    outs = pl.pallas_call(
        head_block,
        in_specs=[
            pl.BlockSpec(memory_space=pltpu.SMEM),
            pl.BlockSpec(memory_space=pltpu.VMEM),
            pl.BlockSpec(memory_space=pltpu.VMEM),
            in_hbm,
            in_hbm,
        ],
        out_shape=[pltpu.VMEM(block, jnp.bfloat16)] * (2 * side - 2),
        scratch_shapes=[
            pltpu.VMEM((side, depth, side * width), jnp.bfloat16),
            pltpu.SemaphoreType.DMA((side, 2 * side)),
        ],
        compiler_params=pltpu.CompilerParams(vmem_limit_bytes=HEAD_VMEM),
        interpret=INTERPRET,
        name="head_partials",
    )(
        place,
        near_by(gathered),
        near_by(gain),
        far_off(near_weight),
        far_off(far_weight),
    )
    return outs[: side - 1], outs[side - 1 :]


def partner_weights_block(sizes, place, near_weight, far_weight, out_x, out_y, held, sems, sems_out):
    side, cores, width = sizes
    rows_here = near_weight.shape[0]
    x_at, y_at, core_at = place[0], place[1], place[2]
    copies = []
    for t in range(side):
        places = (
            ((x_at + side // 2) % side, (y_at + t) % side),
            ((x_at + t) % side, (y_at + side // 2) % side),
        )
        for way, (x_to, y_to) in enumerate(places):
            column = pl.multiple_of(((x_to * side + y_to) * cores + core_at) * width, width)
            for k, weight in enumerate((near_weight, far_weight)):
                copy = pltpu.make_async_copy(
                    weight.at[:, pl.ds(column, width)],
                    held.at[way, pl.ds(k * rows_here, rows_here), pl.ds(t * width, width)],
                    sems.at[way, k, t],
                )
                copy.start()
                copies.append(copy)
    for copy in copies:
        copy.wait()
    stores = [
        pltpu.make_async_copy(held.at[way], out, sems_out.at[way])
        for way, out in enumerate((out_x, out_y))
    ]
    for copy in stores:
        copy.start()
    for copy in stores:
        copy.wait()


def partner_weights(near_weight, far_weight, place, side, cores):
    rows_here, columns = near_weight.shape
    width = columns // (side * side * cores)
    shape = (cores * rows_here, side * width)
    in_hbm = pl.BlockSpec(memory_space=pltpu.HBM)
    return pl.pallas_call(
        functools.partial(partner_weights_block, (side, cores, width)),
        in_specs=[pl.BlockSpec(memory_space=pltpu.SMEM), in_hbm, in_hbm],
        out_specs=[in_hbm, in_hbm],
        out_shape=[pltpu.HBM(shape, jnp.bfloat16)] * 2,
        scratch_shapes=[
            pltpu.VMEM((2, *shape), jnp.bfloat16),
            pltpu.SemaphoreType.DMA((2, cores, side)),
            pltpu.SemaphoreType.DMA((2,)),
        ],
        compiler_params=pltpu.CompilerParams(vmem_limit_bytes=ATTEND_VMEM),
        interpret=INTERPRET,
        name="partner_weights",
    )(place, far_off(near_weight), far_off(far_weight))


def head_partner_block(core, rows_x, rows_y, gain_x, gain_y, weight_x, weight_y, *outs):
    weights = (weight_x, weight_y)
    rows_here = rows_x.shape[-1] // 2
    first_core = core[0] == 0
    for way, (rows, gain) in enumerate(((rows_x, gain_x), (rows_y, gain_y))):
        side, tall, width = outs[way].shape
        ordered = in_order(rows)
        half = ordered.shape[0]
        line = jnp.broadcast_to(squares_line(ordered, gain[...]), (tall - half, half))
        tail = jnp.concatenate(
            [line, jnp.zeros((tall - half, width - half), jnp.float32)], axis=1
        )
        sides = (ordered[:, :rows_here], ordered[:, rows_here:])
        near = jnp.where(first_core, sides[0], sides[1])
        far = jnp.where(first_core, sides[1], sides[0])
        features = jnp.concatenate([near, far], axis=1).astype(jnp.bfloat16)
        product = jnp.dot(features, weights[way][...], preferred_element_type=jnp.float32)
        for t in range(side):
            outs[way][t, :half] = product[:, t * width : (t + 1) * width]
            outs[way][t, half:] = tail


def head_partner(rows_x, rows_y, gain_x, gain_y, weight_x, weight_y, core_at, side):
    depth, columns = weight_x.shape
    half = rows_x.size // depth
    block = (side, half + 8, columns // side)
    in_vmem = pl.BlockSpec(memory_space=pltpu.VMEM)
    return pl.pallas_call(
        head_partner_block,
        in_specs=[pl.BlockSpec(memory_space=pltpu.SMEM), *[in_vmem] * 6],
        out_shape=[pltpu.VMEM(block, jnp.float32)] * 2,
        compiler_params=pltpu.CompilerParams(vmem_limit_bytes=ATTEND_VMEM),
        interpret=INTERPRET,
        name="head_partner",
    )(
        core_at.astype(jnp.int32)[None],
        *(near_by(x) for x in (rows_x, rows_y, gain_x, gain_y, weight_x, weight_y)),
    )


def summed_along(parts, axis):
    arrived = [shifted(parts[k], axis, k) for k in range(1, len(parts))]
    total = parts[0].astype(jnp.float32)
    for piece in arrived:
        total = total + piece.astype(jnp.float32)
    return total


def summed_near(parts, partner, axis):
    side = lax.axis_size(axis)
    arrived = [shifted(parts[-1 if k > 1 else 1], axis, k) for k in (1, side - 1)]
    total = parts[0].astype(jnp.float32) + partner
    for piece in arrived:
        total = total + piece.astype(jnp.float32)
    return total


def joined_all(top, total, axes):
    for axis in axes:
        pieces = sent_to_all(jnp.stack([top, total]), axis)
        tops = pieces[:, 0]
        top = jnp.max(tops, axis=0)
        total = jnp.sum(pieces[:, 1] * jnp.exp(tops - top[None]), axis=0)
    return top, total


def local(
    stream,
    input_gain,
    query_bias,
    query_weight,
    out_weight,
    page_cache,
    page_table,
    lengths,
    final_gain,
    head_weight,
):
    side, cores, batches = lax.axis_size("mp_0"), lax.axis_size("mp_2"), lax.axis_size("batch")
    members = side * side * cores
    x_at, y_at, core_at = lax.axis_index("mp_0"), lax.axis_index("mp_1"), lax.axis_index("mp_2")
    batch_at = lax.axis_index("batch")
    first_core = core_at == 0
    seqs, features_here = stream.shape
    full_width = features_here * members
    seq_count = page_table.shape[0]
    head_size = page_cache.shape[-1]

    far_head_weight = shifted(head_weight, "mp_2", 1)
    far_out_weight = shifted(out_weight, "mp_2", 1)

    both_out = jnp.concatenate(
        [
            jnp.where(first_core, out_weight, far_out_weight),
            jnp.where(first_core, far_out_weight, out_weight),
        ],
        axis=1,
    )
    both_out = lax.optimization_barrier(both_out)
    parts = query_parts(stream, input_gain, query_weight).reshape(members, seq_count, -1)
    parts = lax.all_to_all(parts, MP, split_axis=0, concat_axis=0, tiled=True)
    owners = token_owners(page_table, lengths, *page_cache.shape[2:4])
    cosines, sines = turns(lengths - 1, head_size)
    bias = jnp.broadcast_to(query_bias[None], (seq_count, query_bias.shape[0]))
    table = jnp.concatenate([bias, cosines, sines], axis=1)
    sums = jnp.sum(parts.astype(jnp.float32), axis=0)
    attended = attend(
        sums, table, owners, page_cache, full_width, side * side
    )

    mine = lax.all_to_all(attended, XY, 0, 0, tiled=True)
    place = jnp.stack([x_at, y_at, core_at]).astype(jnp.int32)
    weight_x, weight_y = partner_weights(head_weight, far_head_weight, place, side, cores)
    weight_x = shifted(weight_x, "mp_0", side // 2)
    weight_y = shifted(weight_y, "mp_1", side // 2)
    mine = mine.reshape(side * side * seq_count, -1)
    partial_out = jnp.dot(mine, both_out, preferred_element_type=jnp.float32).astype(jnp.bfloat16)
    per_batch = side * side // batches
    arrived = lax.all_to_all(
        partial_out.reshape(batches, per_batch * seq_count, -1),
        "batch",
        split_axis=0,
        concat_axis=0,
        tiled=True,
    )
    rows = stream.reshape(batches, per_batch, cores, seq_count, features_here)
    rows = lax.dynamic_index_in_dim(rows, batch_at, 0, keepdims=False)

    def of_core(core):
        taken = lax.dynamic_index_in_dim(rows, core, 1, keepdims=False).reshape(-1, features_here)
        return jnp.concatenate([taken.astype(jnp.float32), final_gain[None]], axis=0)

    near_rows = of_core(core_at)
    far_rows = shifted(of_core(1 - core_at), "mp_2", 1)
    both = jnp.concatenate(
        [jnp.where(first_core, near_rows, far_rows), jnp.where(first_core, far_rows, near_rows)],
        axis=1,
    )
    residual = both[:-1] + jnp.sum(arrived.astype(jnp.float32), axis=0)
    payload = (residual * both[-1:]).astype(jnp.bfloat16)
    gathered = sent_to_all(payload, BATCH_CORE)
    gathered = gathered.reshape(batches, cores, per_batch, seq_count, -1)
    rows_x = shifted(gathered[: batches // 2], "mp_0", side // 2)
    rows_y = shifted(gathered[batches // 2 :], "mp_1", side // 2)
    gain = both[-1:]
    gain_x = shifted(gain, "mp_0", side // 2)
    gain_y = shifted(gain, "mp_1", side // 2)
    upper, lower = head_partials(gathered, gain, head_weight, far_head_weight, place, side)
    partner_x, partner_y = head_partner(
        rows_x, rows_y, gain_x, gain_y, weight_x, weight_y, core_at, side
    )
    upper = summed_near(upper, partner_x, "mp_0").astype(jnp.bfloat16)
    lower = summed_near(lower, partner_y, "mp_1").astype(jnp.bfloat16)
    upper = summed_along([upper[k] for k in range(side)], "mp_1")
    lower = summed_along([lower[k] for k in range(side)], "mp_0")

    def rescaled(total):
        half = seqs // 2
        squares = total[half, :half] + total[half, half : 2 * half]
        return total[:half] * lax.rsqrt(squares / full_width + EPS)[:, None]

    logits = jnp.concatenate([rescaled(upper), rescaled(lower)], axis=0)

    local_top = jnp.max(logits, axis=1)
    local_sum = jnp.sum(jnp.exp(logits - local_top[:, None]), axis=1)
    highest, summed = joined_all(local_top, local_sum, (MP, "batch"))
    return (logits, jnp.log(summed) + highest)


def solution(mesh):
    torus = Mesh(
        mesh.devices.reshape(mesh.shape["batch"], 4, 4, 2), ("batch", "mp_0", "mp_1", "mp_2")
    )
    in_specs = (
        P(None, MP),
        P(MP),
        P("batch"),
        P(MP, "batch"),
        P("batch", MP),
        P(None, "batch", MP, None, None),
        P(MP, None),
        P(MP),
        P(MP),
        P(MP, "batch"),
    )
    out_specs = (P(None, BATCH_MP), P())

    def step(*args):
        return local(*args)

    step = jax.shard_map(step, mesh=torus, in_specs=in_specs, out_specs=out_specs, check_vma=False)
    return step
```
